64 devices in a mesh: dp: 4 (over x, y), sp: 16 (over z, core).
Axes of the slice: x: 2, y: 2, z: 8, core: 2. Of those that a mesh axis runs over, the one named last changes fastest.
The devices are a block of a 4x4x8 slice.
Arguments:
- z_points: bfloat16 [131072, 512], P(('dp', 'sp')), parts along dimension 0
- x_points: bfloat16 [32768, 512], P(('dp', 'sp')), parts along dimension 0
- rhs_vals: bfloat16 [32768, 32], P(('dp', 'sp')), parts along dimension 0
- block_mask: int32 [64, 16], P(('dp', 'sp')), parts along dimension 0
- length_scale: float32 [1], replicated
- out_scale: float32 [1], replicated
Outputs:
- output: float32 [131072, 32], P(('dp', 'sp')), parts along dimension 0
There are 4 independent parts. The reference program is written for one: setup_inputs(seed, part) draws one part's arguments, and reference() takes and returns one part's arrays. A program takes and returns all parts, laid end to end along the dimension named above; an argument that names none is the same for every part.
All inputs are finite; a program needn't handle non-finite values.
Results may differ from the reference program's by a relative error of at most 0.001.
Values are sent between devices in bfloat16 or wider.
A program may use at most 768 MiB of HBM per device.

```python
import jax
import jax.numpy as jnp
from jax import lax

D = 512
R = 32
SP = 16
TGT_DEV = 2048
SRC_DEV = 512
CLUSTERS = 8
M_TGT = SP * TGT_DEV
N_SRC = SP * SRC_DEV


def draw_mask(mask_key):
    key_a, key_b = jax.random.split(mask_key)
    mask_draws = jax.random.randint(key_a, (SP, SP), 0, SP)
    limits = jax.random.randint(key_b, (SP, 1), 1, SP + 1)
    on_diag = jnp.arange(SP)[:, None] == jnp.arange(SP)[None, :]
    return jnp.where((mask_draws < limits) | on_diag, 1, 0).astype(jnp.int32)


def setup_inputs(seed: int = 0, part: int = 0) -> dict:
    base_key = jax.random.key(seed)
    shared_key, part_base = jax.random.split(base_key)
    part_key = jax.random.fold_in(part_base, part)
    key_list = jax.random.split(part_key, 9)
    centers = jax.random.normal(key_list[0], (CLUSTERS, D), jnp.float32)
    z_labels = jax.random.randint(key_list[1], (M_TGT,), 0, CLUSTERS)
    x_labels = jax.random.randint(key_list[2], (N_SRC,), 0, CLUSTERS)
    z_vals = centers[z_labels] + 0.5 * jax.random.normal(key_list[3], (M_TGT, D), jnp.float32)
    x_vals = centers[x_labels] + 0.5 * jax.random.normal(key_list[4], (N_SRC, D), jnp.float32)
    col_mean = jax.random.uniform(key_list[5], (1, R), jnp.float32, minval=0.5, maxval=1.5)
    cluster_offs = jax.random.normal(key_list[6], (CLUSTERS, R), jnp.float32)
    rhs_noise = jax.random.normal(key_list[7], (N_SRC, R), jnp.float32)
    rhs = (col_mean + cluster_offs[x_labels] + rhs_noise) * (4.0 / N_SRC)
    block_mask = draw_mask(key_list[8])
    scale_keys = jax.random.split(shared_key)
    length_scale = jnp.sqrt(D * jax.random.uniform(scale_keys[0], (1,), jnp.float32, minval=0.8, maxval=1.4))
    out_scale = jax.random.uniform(scale_keys[1], (1,), jnp.float32, minval=0.5, maxval=1.5)
    return {
        "z_points": z_vals.astype(jnp.bfloat16),
        "x_points": x_vals.astype(jnp.bfloat16),
        "rhs_vals": rhs.astype(jnp.bfloat16),
        "block_mask": block_mask,
        "length_scale": length_scale,
        "out_scale": out_scale,
    }


def reference(z_points, x_points, rhs_vals, block_mask, length_scale, out_scale):
    ell_sq = length_scale[0] * length_scale[0]
    x_f32 = x_points.astype(jnp.float32)
    x_norm = jnp.sum(x_f32 * x_f32, axis=1)
    v_blocks = rhs_vals.reshape(SP, SRC_DEV, R)
    z_blocks = z_points.reshape(SP, TGT_DEV, D)

    def one_block(block_in):
        z_rows, mask_row = block_in
        z_f32 = z_rows.astype(jnp.float32)
        z_norm = jnp.sum(z_f32 * z_f32, axis=1)
        gram_mat = jnp.dot(z_rows, x_points.T, preferred_element_type=jnp.float32)
        sq_dist = jnp.maximum(z_norm[:, None] + x_norm[None, :] - 2.0 * gram_mat, 0.0)
        kern_mat = (out_scale[0] * jnp.exp(-sq_dist / (2.0 * ell_sq))).astype(jnp.bfloat16)
        v_masked = (v_blocks * mask_row[:, None, None].astype(jnp.bfloat16)).reshape(N_SRC, R)
        return jnp.dot(kern_mat, v_masked, preferred_element_type=jnp.float32)

    y_blocks = lax.map(one_block, (z_blocks, block_mask))
    return y_blocks.reshape(M_TGT, R)
```

```python
import functools
import math

import jax
import jax.numpy as jnp
from jax import lax
from jax.experimental import pallas as pl
from jax.experimental.pallas import tpu as pltpu
from jax.sharding import PartitionSpec as P

F32 = jnp.float32
BF16 = jnp.bfloat16
MESH = pl.DeviceIdType.MESH
LOG2_E = math.log2(math.e)
TILE = 256
LANES = 128


def kernel(n_dev, z_hbm, x_hbm, v_hbm, mask_hbm, ell_hbm, scl_hbm, y_ref,
           z_in, zt, xs, v_in, nzh, crow, mask_s, ell_s, scl_s,
           load_sem, ring_send, ring_recv, sib_send, sib_recv, own_send, own_recv):
    n_chip = n_dev // 2
    n_step = n_chip - 1
    mz, d = z_hbm.shape
    nx, r = v_hbm.shape
    half_rows = nx // 2
    vrows = r * half_rows // d
    q_rows = half_rows // 2
    pieces = ((0, vrows + q_rows), (vrows + q_rows, q_rows))

    me = lax.axis_index("sp")
    chip, core = me // 2, me % 2
    right = ((chip + 1) % n_chip) * 2 + core
    left = ((chip + n_chip - 1) % n_chip) * 2 + core
    sib = chip * 2 + (1 - core)

    barrier = pltpu.get_barrier_semaphore()
    for peer in (right, left, sib):
        pl.semaphore_signal(barrier, inc=1, device_id={"sp": peer}, device_id_type=MESH)

    loads = [
        pltpu.make_async_copy(v_hbm, v_in, load_sem.at[0]),
        pltpu.make_async_copy(x_hbm.at[pl.ds(0, half_rows)], xs.at[me, 0, pl.ds(vrows, half_rows)], load_sem.at[1]),
        pltpu.make_async_copy(x_hbm.at[pl.ds(half_rows, half_rows)], xs.at[me, 1, pl.ds(vrows, half_rows)], load_sem.at[2]),
        pltpu.make_async_copy(z_hbm, z_in, load_sem.at[3]),
        pltpu.make_async_copy(mask_hbm, mask_s, load_sem.at[4]),
        pltpu.make_async_copy(ell_hbm, ell_s, load_sem.at[5]),
        pltpu.make_async_copy(scl_hbm, scl_s, load_sem.at[6]),
    ]
    for load in loads:
        load.start()

    loads[0].wait()
    vt = v_in[...].astype(F32).T.astype(BF16)
    for half in range(2):
        cols = vt[:, half * half_rows:(half + 1) * half_rows]
        xs[me, half, 0:vrows, :] = jnp.concatenate([cols[b * vrows:(b + 1) * vrows] for b in range(r // vrows)], axis=1)

    def remote(src_dst, send_sem, recv_sem, peer):
        return pltpu.make_async_remote_copy(
            src_ref=src_dst, dst_ref=src_dst, send_sem=send_sem, recv_sem=recv_sem,
            device_id={"sp": peer}, device_id_type=MESH)

    def piece(j, half, q):
        return xs.at[j, half, pl.ds(*pieces[q])]

    def to_right(s, q):
        j = ((chip + n_chip - s // 2) % n_chip) * 2 + core
        return remote(piece(j, s % 2, q), ring_send.at[0, s, q], ring_recv.at[0, s, q], right)

    def to_left(s, q):
        j = ((chip + s // 2) % n_chip) * 2 + core
        return remote(piece(j, 1 - s % 2, q), ring_send.at[1, s, q], ring_recv.at[1, s, q], left)

    def source(u, c):
        h = u // 2 + 1
        return (((chip + n_chip - h) % n_chip) * 2 + c, u % 2), (((chip + h) % n_chip) * 2 + c, 1 - u % 2)

    def from_ring(u, q):
        a, b = source(u, core)
        return (remote(piece(*a, q), ring_send.at[0, u, q], ring_recv.at[0, u, q], left),
                remote(piece(*b, q), ring_send.at[1, u, q], ring_recv.at[1, u, q], right))

    def sibling(u, q, c):
        a, b = source(u, c)
        return (remote(piece(*a, q), sib_send.at[0, u, q], sib_recv.at[0, u, q], sib),
                remote(piece(*b, q), sib_send.at[1, u, q], sib_recv.at[1, u, q], sib))

    def own(j, half):
        return remote(xs.at[j, half], own_send.at[half], own_recv.at[half], sib)

    loads[1].wait()
    loads[2].wait()
    pl.semaphore_wait(barrier, 3)
    for s in range(2):
        for q in range(2):
            to_right(s, q).start()
            to_left(s, q).start()
    for half in range(2):
        own(me, half).start()

    loads[5].wait()
    loads[6].wait()
    loads[4].wait()
    ell = jnp.full((8, TILE), ell_s[0], F32)
    crow[...] = (-LOG2_E) / (ell * ell)
    loads[3].wait()
    for t in range(mz // TILE):
        zt_t = z_in[t * TILE:(t + 1) * TILE, :].T
        zt[:, t * TILE:(t + 1) * TILE] = zt_t
        zf = zt_t.astype(F32)
        nzh[:, t * TILE:(t + 1) * TILE] = jnp.broadcast_to(
            0.5 * jnp.sum(zf * zf, axis=0, keepdims=True), (8, TILE))
    y_ref[...] = jnp.zeros_like(y_ref)

    def weighted(j, half, lane0, width):
        v_rows = jnp.concatenate(
            [xs[j, half, 0:vrows, b * half_rows + lane0:b * half_rows + lane0 + width] for b in range(r // vrows)], axis=0)
        return (v_rows.astype(F32) * mask_s[0, j].astype(F32)).astype(BF16)

    def accumulate(x, vt_x):
        xf = x.astype(F32)
        nxh = 0.5 * jnp.sum(xf * xf, axis=1, keepdims=True)
        scale = scl_s[0]
        for t in range(mz // TILE):
            cols = slice(t * TILE, (t + 1) * TILE)
            gram = jnp.dot(x, zt[:, cols], preferred_element_type=F32)
            half_dist = jnp.maximum(nzh[0:1, cols] + nxh - gram, 0.0)
            kern = (scale * jnp.exp2(half_dist * crow[0:1, :])).astype(BF16)
            y_ref[:, cols] += jnp.dot(vt_x, kern, preferred_element_type=F32)

    def use_half(j, half):
        accumulate(xs[j, half, vrows:vrows + half_rows, :], weighted(j, half, 0, half_rows))

    def use_pair(u, q, c):
        a, b = source(u, c)
        x = jnp.concatenate([xs[a[0], a[1], pl.ds(vrows + q * q_rows, q_rows), :],
                             xs[b[0], b[1], pl.ds(vrows + q * q_rows, q_rows), :]], axis=0)
        vt_x = jnp.concatenate([weighted(*a, q * q_rows, q_rows), weighted(*b, q * q_rows, q_rows)], axis=1)
        accumulate(x, vt_x)

    @pl.loop(0, 2)
    def _(half):
        use_half(me, half)

    @pl.loop(0, 2)
    def _(half):
        own(sib, half).wait_recv()
        use_half(sib, half)

    @pl.loop(0, n_step)
    def _(u):
        for q in range(2):
            ring = from_ring(u, q)
            to_sib = sibling(u, q, core)
            for k in range(2):
                ring[k].wait_recv()

                @pl.when(u < n_step - 2)
                def _():
                    (to_right, to_left)[k](u + 2, q).start()

                to_sib[k].start()
            use_pair(u, q, core)
            for copy in sibling(u, q, 1 - core):
                copy.wait_recv()
            use_pair(u, q, 1 - core)

    for half in range(2):
        own(me, half).wait_send()

    @pl.loop(0, n_step)
    def _(u):
        for q in range(2):
            to_right(u, q).wait_send()
            to_left(u, q).wait_send()
            for copy in sibling(u, q, core):
                copy.wait_send()


def solution(mesh):
    n_dev = mesh.shape["sp"]
    n_step = n_dev // 2 - 1
    row_spec = P(("dp", "sp"), None)

    def local_fn(z_rows, x_rows, v_rows, mask_row, length_scale, out_scale):
        mz, d = z_rows.shape
        nx, r = v_rows.shape
        slot_rows = nx // 2 + r * nx // 2 // d
        dma = pltpu.SemaphoreType.DMA
        y_t = pl.pallas_call(
            functools.partial(kernel, n_dev),
            name="ring_predict",
            out_shape=jax.ShapeDtypeStruct((r, mz), F32),
            in_specs=[pl.BlockSpec(memory_space=pl.ANY)] * 6,
            out_specs=pl.BlockSpec(memory_space=pltpu.VMEM),
            scratch_shapes=[
                pltpu.VMEM((mz, d), BF16),
                pltpu.VMEM((d, mz), BF16),
                pltpu.VMEM((n_dev, 2, slot_rows, d), BF16),
                pltpu.VMEM((nx, r), BF16),
                pltpu.VMEM((8, mz), F32),
                pltpu.VMEM((8, TILE), F32),
                pltpu.SMEM((1, n_dev), jnp.int32),
                pltpu.SMEM((1,), F32),
                pltpu.SMEM((1,), F32),
                dma((7,)),
                dma((2, n_step, 2)), dma((2, n_step, 2)),
                dma((2, n_step, 2)), dma((2, n_step, 2)),
                dma((2,)), dma((2,)),
            ],
            compiler_params=pltpu.CompilerParams(
                collective_id=0, has_side_effects=True, vmem_limit_bytes=60 * 1024 * 1024),
        )(z_rows, x_rows, v_rows, mask_row, length_scale, out_scale)
        return y_t.T

    return jax.shard_map(local_fn, mesh=mesh, in_specs=(row_spec, row_spec, row_spec, row_spec, P(None), P(None)), out_specs=row_spec, check_vma=False)
```

```python
import functools
import math

import jax
import jax.numpy as jnp
from jax import lax
from jax.experimental import pallas as pl
from jax.experimental.pallas import tpu as pltpu
from jax.sharding import PartitionSpec as P

F32 = jnp.float32
BF16 = jnp.bfloat16
MESH = pl.DeviceIdType.MESH
LOG2_E = math.log2(math.e)
TILE = 512
LANES = 128


def kernel(n_dev, z_hbm, x_hbm, v_hbm, mask_hbm, ell_hbm, scl_hbm, y_ref,
           z_in, zt, xs, nzh, crow, mask_s, ell_s, scl_s,
           nx_s, load_sem, ring_send, ring_recv, sib_send, sib_recv, own_send, own_recv):
    n_chip = n_dev // 2
    n_step = n_chip - 1
    mz, d = z_hbm.shape
    r, nx = v_hbm.shape
    half_rows = nx // 2
    vrows = r * half_rows // d
    q_rows = half_rows // 2
    pieces = ((0, vrows + q_rows), (vrows + q_rows, q_rows))

    me = lax.axis_index("sp")
    chip, core = me // 2, me % 2
    right = ((chip + 1) % n_chip) * 2 + core
    left = ((chip + n_chip - 1) % n_chip) * 2 + core
    sib = chip * 2 + (1 - core)

    barrier = pltpu.get_barrier_semaphore()
    for peer in (right, left, sib):
        pl.semaphore_signal(barrier, inc=1, device_id={"sp": peer}, device_id_type=MESH)

    loads = [pltpu.make_async_copy(x_hbm.at[pl.ds(half * half_rows, half_rows)],
                                   xs.at[me, half, pl.ds(vrows, half_rows)], load_sem.at[half]) for half in range(2)]
    loads += [pltpu.make_async_copy(v_hbm.at[pl.ds(b * vrows, vrows), pl.ds(half * half_rows, half_rows)],
                                    xs.at[me, half, pl.ds(0, vrows), pl.ds(b * half_rows, half_rows)],
                                    load_sem.at[2 + 2 * half + b]) for half in range(2) for b in range(2)]
    n_own = len(loads)
    loads += [
        pltpu.make_async_copy(mask_hbm, mask_s, load_sem.at[n_own]),
        pltpu.make_async_copy(ell_hbm, ell_s, load_sem.at[n_own + 1]),
        pltpu.make_async_copy(scl_hbm, scl_s, load_sem.at[n_own + 2]),
        pltpu.make_async_copy(z_hbm, z_in, load_sem.at[n_own + 3]),
    ]
    for load in loads:
        load.start()

    def remote(src_dst, send_sem, recv_sem, peer):
        return pltpu.make_async_remote_copy(
            src_ref=src_dst, dst_ref=src_dst, send_sem=send_sem, recv_sem=recv_sem,
            device_id={"sp": peer}, device_id_type=MESH)

    def piece(j, half, q):
        return xs.at[j, half, pl.ds(*pieces[q])]

    def to_right(s, q):
        j = ((chip + n_chip - s // 2) % n_chip) * 2 + core
        return remote(piece(j, s % 2, q), ring_send.at[0, s, q], ring_recv.at[0, s, q], right)

    def to_left(s, q):
        j = ((chip + s // 2) % n_chip) * 2 + core
        return remote(piece(j, 1 - s % 2, q), ring_send.at[1, s, q], ring_recv.at[1, s, q], left)

    def source(u, c):
        h = u // 2 + 1
        return (((chip + n_chip - h) % n_chip) * 2 + c, u % 2), (((chip + h) % n_chip) * 2 + c, 1 - u % 2)

    def from_ring(u, q):
        a, b = source(u, core)
        return (remote(piece(*a, q), ring_send.at[0, u, q], ring_recv.at[0, u, q], left),
                remote(piece(*b, q), ring_send.at[1, u, q], ring_recv.at[1, u, q], right))

    def sibling(u, q, c):
        a, b = source(u, c)
        return (remote(piece(*a, q), sib_send.at[0, u, q], sib_recv.at[0, u, q], sib),
                remote(piece(*b, q), sib_send.at[1, u, q], sib_recv.at[1, u, q], sib))

    def own(j, half):
        return remote(xs.at[j, half], own_send.at[half], own_recv.at[half], sib)

    for load in loads[:n_own]:
        load.wait()
    pl.semaphore_wait(barrier, 3)
    for s in range(2):
        for q in range(2):
            to_right(s, q).start()
            to_left(s, q).start()
    for half in range(2):
        own(me, half).start()

    for load in loads[n_own:]:
        load.wait()
    ell = jnp.full((8, TILE), ell_s[0], F32)
    crow[...] = (-LOG2_E) / (ell * ell)
    for t in range(mz // TILE):
        zt_t = z_in[t * TILE:(t + 1) * TILE, :].T
        zt[:, t * TILE:(t + 1) * TILE] = zt_t
        zf = zt_t.astype(F32)
        nzh[:, t * TILE:(t + 1) * TILE] = jnp.broadcast_to(
            0.5 * jnp.sum(zf * zf, axis=0, keepdims=True), (8, TILE))
    y_ref[...] = jnp.zeros_like(y_ref)

    def weighted(j, half, lane0, width):
        v_rows = jnp.concatenate(
            [xs[j, half, 0:vrows, b * half_rows + lane0:b * half_rows + lane0 + width] for b in range(r // vrows)], axis=0)
        return (v_rows.astype(F32) * mask_s[0, j].astype(F32)).astype(BF16)

    def accumulate(x, vt_x):
        xf = x.astype(F32)
        nx_s[...] = jnp.broadcast_to(0.5 * jnp.sum(xf * xf, axis=1, keepdims=True), nx_s.shape)
        scale = scl_s[0]
        tiles = [slice(t * TILE, (t + 1) * TILE) for t in range(mz // TILE)]
        ahead = jnp.dot(x, zt[:, tiles[0]], preferred_element_type=F32)
        for t, cols in enumerate(tiles):
            gram = ahead
            if t + 1 < len(tiles):
                ahead = jnp.dot(x, zt[:, tiles[t + 1]], preferred_element_type=F32)
            half_dist = jnp.maximum(nzh[0:1, cols] + jnp.concatenate([nx_s[...]] * (TILE // LANES), axis=1) - gram, 0.0)
            kern = (scale * jnp.exp2(half_dist * crow[0:1, :])).astype(BF16)
            y_ref[:, cols] += jnp.dot(vt_x, kern, preferred_element_type=F32)

    def use_half(j, half):
        accumulate(xs[j, half, vrows:vrows + half_rows, :], weighted(j, half, 0, half_rows))

    def use_pair(u, q, c):
        a, b = source(u, c)
        x = jnp.concatenate([xs[a[0], a[1], pl.ds(vrows + q * q_rows, q_rows), :],
                             xs[b[0], b[1], pl.ds(vrows + q * q_rows, q_rows), :]], axis=0)
        vt_x = jnp.concatenate([weighted(*a, q * q_rows, q_rows), weighted(*b, q * q_rows, q_rows)], axis=1)
        accumulate(x, vt_x)

    @pl.loop(0, 2)
    def _(half):
        use_half(me, half)

    @pl.loop(0, 2)
    def _(half):
        own(sib, half).wait_recv()
        use_half(sib, half)

    @pl.loop(0, n_step)
    def _(u):
        for q in range(2):
            ring = from_ring(u, q)
            to_sib = sibling(u, q, core)
            for k in range(2):
                ring[k].wait_recv()

                @pl.when(u < n_step - 2)
                def _():
                    (to_right, to_left)[k](u + 2, q).start()

                to_sib[k].start()
            use_pair(u, q, core)
            for copy in sibling(u, q, 1 - core):
                copy.wait_recv()
            use_pair(u, q, 1 - core)

    for half in range(2):
        own(me, half).wait_send()

    @pl.loop(0, n_step)
    def _(u):
        for q in range(2):
            to_right(u, q).wait_send()
            to_left(u, q).wait_send()
            for copy in sibling(u, q, core):
                copy.wait_send()


def solution(mesh):
    n_dev = mesh.shape["sp"]
    n_step = n_dev // 2 - 1
    row_spec = P(("dp", "sp"), None)

    def local_fn(z_rows, x_rows, v_rows, mask_row, length_scale, out_scale):
        mz, d = z_rows.shape
        nx, r = v_rows.shape
        slot_rows = nx // 2 + r * nx // 2 // d
        dma = pltpu.SemaphoreType.DMA
        y_t = pl.pallas_call(
            functools.partial(kernel, n_dev),
            name="ring_predict",
            out_shape=jax.ShapeDtypeStruct((r, mz), F32),
            in_specs=[pl.BlockSpec(memory_space=pl.ANY)] * 6,
            out_specs=pl.BlockSpec(memory_space=pltpu.VMEM),
            scratch_shapes=[
                pltpu.VMEM((mz, d), BF16),
                pltpu.VMEM((d, mz), BF16),
                pltpu.VMEM((n_dev, 2, slot_rows, d), BF16),
                pltpu.VMEM((8, mz), F32),
                pltpu.VMEM((8, TILE), F32),
                pltpu.SMEM((1, n_dev), jnp.int32),
                pltpu.SMEM((1,), F32),
                pltpu.SMEM((1,), F32),
                pltpu.VMEM((nx // 2, LANES), F32),
                dma((10,)),
                dma((2, n_step, 2)), dma((2, n_step, 2)),
                dma((2, n_step, 2)), dma((2, n_step, 2)),
                dma((2,)), dma((2,)),
            ],
            compiler_params=pltpu.CompilerParams(
                collective_id=0, has_side_effects=True, vmem_limit_bytes=60 * 1024 * 1024),
        )(z_rows, x_rows, v_rows.T, mask_row, length_scale, out_scale)
        return y_t.T

    return jax.shard_map(local_fn, mesh=mesh, in_specs=(row_spec, row_spec, row_spec, row_spec, P(None), P(None)), out_specs=row_spec, check_vma=False)
```

```python
import functools
import math

import jax
import jax.numpy as jnp
from jax import lax
from jax.experimental import pallas as pl
from jax.experimental.pallas import tpu as pltpu
from jax.sharding import PartitionSpec as P

F32 = jnp.float32
BF16 = jnp.bfloat16
MESH = pl.DeviceIdType.MESH
LOG2_E = math.log2(math.e)
TILE = 512
LANES = 128


def kernel(n_dev, z_hbm, x_hbm, v_hbm, mask_hbm, ell_s, scl_s, y_ref,
           z_in, zt, xs, nzh, crow, mask_s, nx_s,
           load_sem, ring_send, ring_recv, sib_send, sib_recv, own_send, own_recv):
    n_chip = n_dev // 2
    n_step = n_chip - 1
    mz, d = z_hbm.shape
    r, nx = v_hbm.shape
    half_rows = nx // 2
    vrows = r * half_rows // d
    spans = ((0, half_rows // 2), (half_rows // 2, half_rows // 4), (3 * half_rows // 4, half_rows // 4))
    n_piece = len(spans)

    me = lax.axis_index("sp")
    chip, core = me // 2, me % 2
    right = ((chip + 1) % n_chip) * 2 + core
    left = ((chip + n_chip - 1) % n_chip) * 2 + core
    sib = chip * 2 + (1 - core)

    barrier = pltpu.get_barrier_semaphore()
    for peer in (right, left, sib):
        pl.semaphore_signal(barrier, inc=1, device_id={"sp": peer}, device_id_type=MESH)

    loads = [pltpu.make_async_copy(x_hbm.at[pl.ds(half * half_rows, half_rows)],
                                   xs.at[me, half, pl.ds(vrows, half_rows)], load_sem.at[half]) for half in range(2)]
    loads += [pltpu.make_async_copy(v_hbm.at[pl.ds(b * vrows, vrows), pl.ds(half * half_rows, half_rows)],
                                    xs.at[me, half, pl.ds(0, vrows), pl.ds(b * half_rows, half_rows)],
                                    load_sem.at[2 + 2 * half + b]) for half in range(2) for b in range(2)]
    n_own = len(loads)
    loads += [
        pltpu.make_async_copy(mask_hbm, mask_s, load_sem.at[n_own]),
        pltpu.make_async_copy(z_hbm, z_in, load_sem.at[n_own + 1]),
    ]
    for load in loads:
        load.start()

    def remote(src_dst, send_sem, recv_sem, peer):
        return pltpu.make_async_remote_copy(
            src_ref=src_dst, dst_ref=src_dst, send_sem=send_sem, recv_sem=recv_sem,
            device_id={"sp": peer}, device_id_type=MESH)

    def piece(j, half, q):
        lo, rows = spans[q]
        return xs.at[j, half, pl.ds(vrows + lo, rows) if q else pl.ds(0, vrows + rows)]

    def to_right(s, q):
        j = ((chip + n_chip - s // 2) % n_chip) * 2 + core
        return remote(piece(j, s % 2, q), ring_send.at[0, s, q], ring_recv.at[0, s, q], right)

    def to_left(s, q):
        j = ((chip + s // 2) % n_chip) * 2 + core
        return remote(piece(j, 1 - s % 2, q), ring_send.at[1, s, q], ring_recv.at[1, s, q], left)

    def source(u, c):
        h = u // 2 + 1
        return (((chip + n_chip - h) % n_chip) * 2 + c, u % 2), (((chip + h) % n_chip) * 2 + c, 1 - u % 2)

    def from_ring(u, q):
        a, b = source(u, core)
        return (remote(piece(*a, q), ring_send.at[0, u, q], ring_recv.at[0, u, q], left),
                remote(piece(*b, q), ring_send.at[1, u, q], ring_recv.at[1, u, q], right))

    def sibling(u, q, c):
        a, b = source(u, c)
        return (remote(piece(*a, q), sib_send.at[0, u, q], sib_recv.at[0, u, q], sib),
                remote(piece(*b, q), sib_send.at[1, u, q], sib_recv.at[1, u, q], sib))

    def own(j, half):
        return remote(xs.at[j, half], own_send.at[half], own_recv.at[half], sib)

    def ring_sent(s):
        for q in range(n_piece):
            for k in range(2):
                remote(piece(0, 0, q), ring_send.at[k, s, q], ring_recv.at[k, s, q], right).wait_send()

    def sibling_sent(u, qs):
        for q in qs:
            for k in range(2):
                remote(piece(0, 0, q), sib_send.at[k, u, q], sib_recv.at[k, u, q], sib).wait_send()

    for load in loads[:n_own]:
        load.wait()
    pl.semaphore_wait(barrier, 3)
    for s in range(2):
        for q in range(n_piece):
            to_right(s, q).start()
            to_left(s, q).start()
    for half in range(2):
        own(me, half).start()

    for load in loads[n_own:]:
        load.wait()
    ell = jnp.full((8, TILE), ell_s[0], F32)
    crow[...] = (-LOG2_E) / (ell * ell)
    for t in range(mz // TILE):
        zt_t = z_in[t * TILE:(t + 1) * TILE, :].T
        zt[:, t * TILE:(t + 1) * TILE] = zt_t
        zf = zt_t.astype(F32)
        nzh[:, t * TILE:(t + 1) * TILE] = jnp.broadcast_to(
            0.5 * jnp.sum(zf * zf, axis=0, keepdims=True), (8, TILE))
    y_ref[...] = jnp.zeros_like(y_ref)

    def weighted(j, half, lo, rows):
        v_rows = jnp.concatenate(
            [xs[j, half, 0:vrows, b * half_rows:(b + 1) * half_rows][:, lo:lo + rows] for b in range(r // vrows)], axis=0)
        return (v_rows.astype(F32) * mask_s[0, j].astype(F32)).astype(BF16)

    def accumulate(x, vt_x):
        rows = x.shape[0]
        xf = x.astype(F32)
        nx_s[0:rows, :] = jnp.broadcast_to(0.5 * jnp.sum(xf * xf, axis=1, keepdims=True), (rows, LANES))
        scale = scl_s[0]
        tiles = [slice(t * TILE, (t + 1) * TILE) for t in range(mz // TILE)]
        ahead = jnp.dot(x, zt[:, tiles[0]], preferred_element_type=F32)
        for t, cols in enumerate(tiles):
            gram = ahead
            if t + 1 < len(tiles):
                ahead = jnp.dot(x, zt[:, tiles[t + 1]], preferred_element_type=F32)
            nxh = jnp.concatenate([nx_s[0:rows, :]] * (TILE // LANES), axis=1)
            half_dist = jnp.maximum(nzh[0:1, cols] + nxh - gram, 0.0)
            kern = (scale * jnp.exp2(half_dist * crow[0:1, :])).astype(BF16)
            y_ref[:, cols] += jnp.dot(vt_x, kern, preferred_element_type=F32)

    def use_half(j, half):
        accumulate(xs[j, half, vrows:vrows + half_rows, :], weighted(j, half, 0, half_rows))

    def use_pair(u, c, lo, rows):
        a, b = source(u, c)
        x = jnp.concatenate([xs[a[0], a[1], pl.ds(vrows + lo, rows), :], xs[b[0], b[1], pl.ds(vrows + lo, rows), :]], axis=0)
        accumulate(x, jnp.concatenate([weighted(*a, lo, rows), weighted(*b, lo, rows)], axis=1))

    @pl.loop(0, 2)
    def _(half):
        use_half(me, half)

    @pl.loop(0, 2)
    def _(half):
        own(sib, half).wait_recv()
        use_half(sib, half)

    def arrive(u, q, forward):
        ring = from_ring(u, q)
        to_sib = sibling(u, q, core)
        for k in range(2):
            ring[k].wait_recv()
            if forward:
                @pl.when(u < n_step - 2)
                def _():
                    (to_right, to_left)[k](u + 2, q).start()

            to_sib[k].start()

    def step(u, groups, forward):
        for qs in groups:
            for q in qs:
                arrive(u, q, forward)
            lo, rows = spans[qs[0]][0], sum(spans[q][1] for q in qs)
            use_pair(u, core, lo, rows)
            for q in qs:
                for copy in sibling(u, q, 1 - core):
                    copy.wait_recv()
            use_pair(u, 1 - core, lo, rows)

    @pl.loop(0, n_step - 1)
    def _(u):
        step(u, ((0,), (1, 2)), True)

        @pl.when(u > 0)
        def _():
            ring_sent(u - 1)
            sibling_sent(u - 1, range(n_piece))

    ring_sent(n_step - 2)
    sibling_sent(n_step - 2, range(n_piece))
    for half in range(2):
        own(me, half).wait_send()
    step(n_step - 1, ((0,), (1,), (2,)), False)
    ring_sent(n_step - 1)
    sibling_sent(n_step - 1, range(n_piece))


def solution(mesh):
    n_dev = mesh.shape["sp"]
    n_step = n_dev // 2 - 1
    row_spec = P(("dp", "sp"), None)

    def local_fn(z_rows, x_rows, v_rows, mask_row, length_scale, out_scale):
        mz, d = z_rows.shape
        nx, r = v_rows.shape
        slot_rows = nx // 2 + r * nx // 2 // d
        dma = pltpu.SemaphoreType.DMA
        y_t = pl.pallas_call(
            functools.partial(kernel, n_dev),
            name="ring_predict",
            out_shape=pltpu.VMEM((r, mz), F32),
            in_specs=[pl.BlockSpec(memory_space=pl.ANY)] * 4 + [pl.BlockSpec(memory_space=pltpu.SMEM)] * 2,
            out_specs=pl.BlockSpec(memory_space=pltpu.VMEM),
            scratch_shapes=[
                pltpu.VMEM((mz, d), BF16),
                pltpu.VMEM((d, mz), BF16),
                pltpu.VMEM((n_dev, 2, slot_rows, d), BF16),
                pltpu.VMEM((8, mz), F32),
                pltpu.VMEM((8, TILE), F32),
                pltpu.SMEM((1, n_dev), jnp.int32),
                pltpu.VMEM((nx // 2, LANES), F32),
                dma((8,)),
                dma((2, n_step, 3)), dma((2, n_step, 3)),
                dma((2, n_step, 3)), dma((2, n_step, 3)),
                dma((2,)), dma((2,)),
            ],
            compiler_params=pltpu.CompilerParams(
                collective_id=0, has_side_effects=True, vmem_limit_bytes=60 * 1024 * 1024),
        )(z_rows, x_rows, v_rows.T, mask_row, length_scale, out_scale)
        return y_t.T

    return jax.shard_map(local_fn, mesh=mesh, in_specs=(row_spec, row_spec, row_spec, row_spec, P(None), P(None)), out_specs=row_spec, check_vma=False)
```

```python
import functools
import math

import jax
import jax.numpy as jnp
from jax import lax
from jax.experimental import pallas as pl
from jax.experimental.pallas import tpu as pltpu
from jax.sharding import PartitionSpec as P

F32 = jnp.float32
BF16 = jnp.bfloat16
MESH = pl.DeviceIdType.MESH
LOG2_E = math.log2(math.e)
TILE = 512
LANES = 128


def kernel(n_dev, z_hbm, x_hbm, v_hbm, mask_hbm, ell_s, scl_s, y_ref,
           z_in, zt, xs, nzh, crow, mask_s, nx_s,
           load_sem, ring_send, ring_recv, sib_send, sib_recv, own_send, own_recv):
    n_chip = n_dev // 2
    n_step = n_chip - 1
    mz, d = z_hbm.shape
    r, nx = v_hbm.shape
    half_rows = nx // 2
    vrows = r * half_rows // d
    spans = ((0, half_rows // 2), (half_rows // 2, half_rows // 4), (3 * half_rows // 4, half_rows // 4))
    n_piece = len(spans)
    last = n_step - 1

    me = lax.axis_index("sp")
    chip, core = me // 2, me % 2
    right = ((chip + 1) % n_chip) * 2 + core
    left = ((chip + n_chip - 1) % n_chip) * 2 + core
    sib = chip * 2 + (1 - core)

    barrier = pltpu.get_barrier_semaphore()
    for peer in (right, left, sib):
        pl.semaphore_signal(barrier, inc=1, device_id={"sp": peer}, device_id_type=MESH)

    loads = [pltpu.make_async_copy(x_hbm.at[pl.ds(half * half_rows, half_rows)],
                                   xs.at[me, half, pl.ds(vrows, half_rows)], load_sem.at[half]) for half in range(2)]
    loads += [pltpu.make_async_copy(v_hbm.at[pl.ds(b * vrows, vrows), pl.ds(half * half_rows, half_rows)],
                                    xs.at[me, half, pl.ds(0, vrows), pl.ds(b * half_rows, half_rows)],
                                    load_sem.at[2 + 2 * half + b]) for half in range(2) for b in range(2)]
    n_own = len(loads)
    loads += [
        pltpu.make_async_copy(mask_hbm, mask_s, load_sem.at[n_own]),
        pltpu.make_async_copy(z_hbm, z_in, load_sem.at[n_own + 1]),
    ]
    for load in loads:
        load.start()

    def remote(src_dst, send_sem, recv_sem, peer):
        return pltpu.make_async_remote_copy(
            src_ref=src_dst, dst_ref=src_dst, send_sem=send_sem, recv_sem=recv_sem,
            device_id={"sp": peer}, device_id_type=MESH)

    def piece(j, half, q, whole):
        if whole:
            return xs.at[j, half]
        lo, rows = spans[q]
        return xs.at[j, half, pl.ds(vrows + lo, rows) if q else pl.ds(0, vrows + rows)]

    def to_right(s, q=0, whole=True):
        j = ((chip + n_chip - s // 2) % n_chip) * 2 + core
        return remote(piece(j, s % 2, q, whole), ring_send.at[0, s, q], ring_recv.at[0, s, q], right)

    def to_left(s, q=0, whole=True):
        j = ((chip + s // 2) % n_chip) * 2 + core
        return remote(piece(j, 1 - s % 2, q, whole), ring_send.at[1, s, q], ring_recv.at[1, s, q], left)

    def source(u, c):
        h = u // 2 + 1
        return (((chip + n_chip - h) % n_chip) * 2 + c, u % 2), (((chip + h) % n_chip) * 2 + c, 1 - u % 2)

    def from_ring(u, q=0, whole=True):
        a, b = source(u, core)
        return (remote(piece(*a, q, whole), ring_send.at[0, u, q], ring_recv.at[0, u, q], left),
                remote(piece(*b, q, whole), ring_send.at[1, u, q], ring_recv.at[1, u, q], right))

    def sibling(u, c, q=0, whole=True):
        a, b = source(u, c)
        return (remote(piece(*a, q, whole), sib_send.at[0, u, q], sib_recv.at[0, u, q], sib),
                remote(piece(*b, q, whole), sib_send.at[1, u, q], sib_recv.at[1, u, q], sib))

    def own(j, half):
        return remote(xs.at[j, half], own_send.at[half], own_recv.at[half], sib)

    def sent(sems, u, q=0, whole=True):
        for k in range(2):
            remote(piece(0, 0, q, whole), sems.at[k, u, q], ring_recv.at[k, u, q], sib).wait_send()

    for load in loads[:n_own]:
        load.wait()
    pl.semaphore_wait(barrier, 3)
    for s in range(2):
        to_right(s).start()
        to_left(s).start()
    for half in range(2):
        own(me, half).start()

    for load in loads[n_own:]:
        load.wait()
    ell = jnp.full((8, TILE), ell_s[0], F32)
    crow[...] = (-LOG2_E) / (ell * ell)
    for t in range(mz // TILE):
        zt_t = z_in[t * TILE:(t + 1) * TILE, :].T
        zt[:, t * TILE:(t + 1) * TILE] = zt_t
        zf = zt_t.astype(F32)
        nzh[:, t * TILE:(t + 1) * TILE] = jnp.broadcast_to(
            0.5 * jnp.sum(zf * zf, axis=0, keepdims=True), (8, TILE))
    y_ref[...] = jnp.zeros_like(y_ref)

    def weighted(j, half, lo, rows):
        v_rows = jnp.concatenate(
            [xs[j, half, 0:vrows, b * half_rows:(b + 1) * half_rows][:, lo:lo + rows] for b in range(r // vrows)], axis=0)
        return (v_rows.astype(F32) * mask_s[0, j].astype(F32)).astype(BF16)

    def accumulate(x, vt_x):
        rows = x.shape[0]
        xf = x.astype(F32)
        nx_s[0:rows, :] = jnp.broadcast_to(0.5 * jnp.sum(xf * xf, axis=1, keepdims=True), (rows, LANES))
        scale = scl_s[0]
        tiles = [slice(t * TILE, (t + 1) * TILE) for t in range(mz // TILE)]
        ahead = jnp.dot(x, zt[:, tiles[0]], preferred_element_type=F32)
        for t, cols in enumerate(tiles):
            gram = ahead
            if t + 1 < len(tiles):
                ahead = jnp.dot(x, zt[:, tiles[t + 1]], preferred_element_type=F32)
            nxh = jnp.concatenate([nx_s[0:rows, :]] * (TILE // LANES), axis=1)
            half_dist = jnp.maximum(nzh[0:1, cols] + nxh - gram, 0.0)
            kern = (scale * jnp.exp2(half_dist * crow[0:1, :])).astype(BF16)
            y_ref[:, cols] += jnp.dot(vt_x, kern, preferred_element_type=F32)

    def use_half(j, half):
        accumulate(xs[j, half, vrows:vrows + half_rows, :], weighted(j, half, 0, half_rows))

    def use_pair(u, c, lo, rows):
        a, b = source(u, c)
        x = jnp.concatenate([xs[a[0], a[1], pl.ds(vrows + lo, rows), :], xs[b[0], b[1], pl.ds(vrows + lo, rows), :]], axis=0)
        accumulate(x, jnp.concatenate([weighted(*a, lo, rows), weighted(*b, lo, rows)], axis=1))

    @pl.loop(0, 2)
    def _(half):
        use_half(me, half)

    @pl.loop(0, 2)
    def _(half):
        own(sib, half).wait_recv()
        use_half(sib, half)

    @pl.loop(0, last)
    def _(u):
        ring, to_sib = from_ring(u), sibling(u, core)
        for k in range(2):
            onward = (to_right, to_left)[k]
            ring[k].wait_recv()

            @pl.when(u < last - 2)
            def _():
                onward(u + 2).start()

            @pl.when(u == last - 2)
            def _():
                for q in range(n_piece):
                    onward(last, q, False).start()

            to_sib[k].start()
        for j, half in source(u, core):
            use_half(j, half)
        for copy in sibling(u, 1 - core):
            copy.wait_recv()
        for j, half in source(u, 1 - core):
            use_half(j, half)

        @pl.when(u > 0)
        def _():
            sent(ring_send, u - 1)
            sent(sib_send, u - 1)

    sent(ring_send, last - 1)
    sent(sib_send, last - 1)
    for half in range(2):
        own(me, half).wait_send()

    def arrive(q):
        ring, to_sib = from_ring(last, q, False), sibling(last, core, q, False)
        for k in range(2):
            ring[k].wait_recv()
            to_sib[k].start()

    def use_sibling(q):
        for copy in sibling(last, 1 - core, q, False):
            copy.wait_recv()
        use_pair(last, 1 - core, *spans[q])

    arrive(0)
    use_pair(last, core, *spans[0])
    use_sibling(0)
    for q in range(1, n_piece):
        arrive(q)
        if q > 1:
            use_sibling(q - 1)
        use_pair(last, core, *spans[q])
    use_sibling(n_piece - 1)
    for q in range(n_piece):
        sent(ring_send, last, q, False)
        sent(sib_send, last, q, False)


def solution(mesh):
    n_dev = mesh.shape["sp"]
    n_step = n_dev // 2 - 1
    row_spec = P(("dp", "sp"), None)

    def local_fn(z_rows, x_rows, v_rows, mask_row, length_scale, out_scale):
        mz, d = z_rows.shape
        nx, r = v_rows.shape
        slot_rows = nx // 2 + r * nx // 2 // d
        dma = pltpu.SemaphoreType.DMA
        y_t = pl.pallas_call(
            functools.partial(kernel, n_dev),
            name="ring_predict",
            out_shape=pltpu.VMEM((r, mz), F32),
            in_specs=[pl.BlockSpec(memory_space=pl.ANY)] * 4 + [pl.BlockSpec(memory_space=pltpu.SMEM)] * 2,
            out_specs=pl.BlockSpec(memory_space=pltpu.VMEM),
            scratch_shapes=[
                pltpu.VMEM((mz, d), BF16),
                pltpu.VMEM((d, mz), BF16),
                pltpu.VMEM((n_dev, 2, slot_rows, d), BF16),
                pltpu.VMEM((8, mz), F32),
                pltpu.VMEM((8, TILE), F32),
                pltpu.SMEM((1, n_dev), jnp.int32),
                pltpu.VMEM((nx // 2, LANES), F32),
                dma((8,)),
                dma((2, n_step, 3)), dma((2, n_step, 3)),
                dma((2, n_step, 3)), dma((2, n_step, 3)),
                dma((2,)), dma((2,)),
            ],
            compiler_params=pltpu.CompilerParams(
                collective_id=0, has_side_effects=True, vmem_limit_bytes=60 * 1024 * 1024),
        )(z_rows, x_rows, v_rows.T, mask_row, length_scale, out_scale)
        return y_t.T

    return jax.shard_map(local_fn, mesh=mesh, in_specs=(row_spec, row_spec, row_spec, row_spec, P(None), P(None)), out_specs=row_spec, check_vma=False)
```

```python
import functools
import math

import jax
import jax.numpy as jnp
from jax import lax
from jax.experimental import pallas as pl
from jax.experimental.pallas import tpu as pltpu
from jax.sharding import PartitionSpec as P

F32 = jnp.float32
BF16 = jnp.bfloat16
MESH = pl.DeviceIdType.MESH
LOG2_E = math.log2(math.e)
TILE = 512
LANES = 128


def kernel(n_dev, z_hbm, x_hbm, v_hbm, mask_hbm, ell_s, scl_s, y_ref,
           z_in, zt, xs, nzh, crow, mask_s, nx_s,
           load_sem, ring_send, ring_recv, sib_send, sib_recv, own_send, own_recv):
    n_chip = n_dev // 2
    n_step = n_chip - 1
    mz, d = z_hbm.shape
    r, nx = v_hbm.shape
    half_rows = nx // 2
    vrows = r * half_rows // d
    spans = ((0, half_rows // 2), (half_rows // 2, 5 * half_rows // 16), (13 * half_rows // 16, 3 * half_rows // 16))
    n_piece = len(spans)
    last = n_step - 1

    me = lax.axis_index("sp")
    chip, core = me // 2, me % 2
    right = ((chip + 1) % n_chip) * 2 + core
    left = ((chip + n_chip - 1) % n_chip) * 2 + core
    sib = chip * 2 + (1 - core)

    barrier = pltpu.get_barrier_semaphore()
    for peer in (right, left, sib):
        pl.semaphore_signal(barrier, inc=1, device_id={"sp": peer}, device_id_type=MESH)

    loads = [pltpu.make_async_copy(x_hbm.at[pl.ds(half * half_rows, half_rows)],
                                   xs.at[me, half, pl.ds(vrows, half_rows)], load_sem.at[half]) for half in range(2)]
    loads += [pltpu.make_async_copy(v_hbm.at[pl.ds(b * vrows, vrows), pl.ds(half * half_rows, half_rows)],
                                    xs.at[me, half, pl.ds(0, vrows), pl.ds(b * half_rows, half_rows)],
                                    load_sem.at[2 + 2 * half + b]) for half in range(2) for b in range(2)]
    n_own = len(loads)
    loads += [
        pltpu.make_async_copy(mask_hbm, mask_s, load_sem.at[n_own]),
        pltpu.make_async_copy(z_hbm, z_in, load_sem.at[n_own + 1]),
    ]
    for load in loads:
        load.start()

    def remote(src_dst, send_sem, recv_sem, peer):
        return pltpu.make_async_remote_copy(
            src_ref=src_dst, dst_ref=src_dst, send_sem=send_sem, recv_sem=recv_sem,
            device_id={"sp": peer}, device_id_type=MESH)

    def piece(j, half, q, whole):
        if whole:
            return xs.at[j, half]
        lo, rows = spans[q]
        return xs.at[j, half, pl.ds(vrows + lo, rows) if q else pl.ds(0, vrows + rows)]

    def to_right(s, q=0, whole=True):
        j = ((chip + n_chip - s // 2) % n_chip) * 2 + core
        return remote(piece(j, s % 2, q, whole), ring_send.at[0, s, q], ring_recv.at[0, s, q], right)

    def to_left(s, q=0, whole=True):
        j = ((chip + s // 2) % n_chip) * 2 + core
        return remote(piece(j, 1 - s % 2, q, whole), ring_send.at[1, s, q], ring_recv.at[1, s, q], left)

    def source(u, c):
        h = u // 2 + 1
        return (((chip + n_chip - h) % n_chip) * 2 + c, u % 2), (((chip + h) % n_chip) * 2 + c, 1 - u % 2)

    def from_ring(u, q=0, whole=True):
        a, b = source(u, core)
        return (remote(piece(*a, q, whole), ring_send.at[0, u, q], ring_recv.at[0, u, q], left),
                remote(piece(*b, q, whole), ring_send.at[1, u, q], ring_recv.at[1, u, q], right))

    def sibling(u, c, q=0, whole=True):
        a, b = source(u, c)
        return (remote(piece(*a, q, whole), sib_send.at[0, u, q], sib_recv.at[0, u, q], sib),
                remote(piece(*b, q, whole), sib_send.at[1, u, q], sib_recv.at[1, u, q], sib))

    def own(j, half):
        return remote(xs.at[j, half], own_send.at[half], own_recv.at[half], sib)

    def sent(sems, u, q=0, whole=True):
        for k in range(2):
            remote(piece(0, 0, q, whole), sems.at[k, u, q], ring_recv.at[k, u, q], sib).wait_send()

    for load in loads[:n_own]:
        load.wait()
    pl.semaphore_wait(barrier, 3)
    for s in range(2):
        to_right(s).start()
        to_left(s).start()
    for half in range(2):
        own(me, half).start()

    for load in loads[n_own:]:
        load.wait()
    ell = jnp.full((8, TILE), ell_s[0], F32)
    crow[...] = (-LOG2_E) / (ell * ell)
    for t in range(mz // TILE):
        zt_t = z_in[t * TILE:(t + 1) * TILE, :].T
        zt[:, t * TILE:(t + 1) * TILE] = zt_t
        zf = zt_t.astype(F32)
        nzh[:, t * TILE:(t + 1) * TILE] = jnp.broadcast_to(
            0.5 * jnp.sum(zf * zf, axis=0, keepdims=True), (8, TILE))
    y_ref[...] = jnp.zeros_like(y_ref)

    def weighted(j, half, lo, rows):
        v_rows = jnp.concatenate(
            [xs[j, half, 0:vrows, b * half_rows:(b + 1) * half_rows][:, lo:lo + rows] for b in range(r // vrows)], axis=0)
        return (v_rows.astype(F32) * mask_s[0, j].astype(F32)).astype(BF16)

    def accumulate(x, vt_x):
        rows = x.shape[0]
        xf = x.astype(F32)
        nx_s[0:rows, :] = jnp.broadcast_to(0.5 * jnp.sum(xf * xf, axis=1, keepdims=True), (rows, LANES))
        scale = scl_s[0]
        tiles = [slice(t * TILE, (t + 1) * TILE) for t in range(mz // TILE)]
        ahead = jnp.dot(x, zt[:, tiles[0]], preferred_element_type=F32)
        for t, cols in enumerate(tiles):
            gram = ahead
            if t + 1 < len(tiles):
                ahead = jnp.dot(x, zt[:, tiles[t + 1]], preferred_element_type=F32)
            nxh = jnp.concatenate([nx_s[0:rows, :]] * (TILE // LANES), axis=1)
            half_dist = jnp.maximum(nzh[0:1, cols] + nxh - gram, 0.0)
            kern = (scale * jnp.exp2(half_dist * crow[0:1, :])).astype(BF16)
            y_ref[:, cols] += jnp.dot(vt_x, kern, preferred_element_type=F32)

    def use_halves(*blocks):
        x = jnp.concatenate([xs[j, half, vrows:vrows + half_rows, :] for j, half in blocks], axis=0)
        accumulate(x, jnp.concatenate([weighted(j, half, 0, half_rows) for j, half in blocks], axis=1))

    def use_pair(u, c, lo, rows):
        a, b = source(u, c)
        x = jnp.concatenate([xs[a[0], a[1], pl.ds(vrows + lo, rows), :], xs[b[0], b[1], pl.ds(vrows + lo, rows), :]], axis=0)
        accumulate(x, jnp.concatenate([weighted(*a, lo, rows), weighted(*b, lo, rows)], axis=1))

    use_halves((me, 0), (me, 1))
    for half in range(2):
        own(sib, half).wait_recv()
    use_halves((sib, 0), (sib, 1))

    @pl.loop(0, last)
    def _(u):
        ring, to_sib = from_ring(u), sibling(u, core)
        for k in range(2):
            onward = (to_right, to_left)[k]
            ring[k].wait_recv()

            @pl.when(u < last - 2)
            def _():
                onward(u + 2).start()

            @pl.when(u == last - 2)
            def _():
                for q in range(n_piece):
                    onward(last, q, False).start()

            to_sib[k].start()
        use_halves(*source(u, core))
        for copy in sibling(u, 1 - core):
            copy.wait_recv()
        use_halves(*source(u, 1 - core))

        @pl.when(u > 0)
        def _():
            sent(ring_send, u - 1)
            sent(sib_send, u - 1)

    sent(ring_send, last - 1)
    sent(sib_send, last - 1)
    for half in range(2):
        own(me, half).wait_send()

    def arrive(q):
        ring, to_sib = from_ring(last, q, False), sibling(last, core, q, False)
        for k in range(2):
            ring[k].wait_recv()
            to_sib[k].start()

    def use_sibling(q):
        for copy in sibling(last, 1 - core, q, False):
            copy.wait_recv()
        use_pair(last, 1 - core, *spans[q])

    arrive(0)
    use_pair(last, core, *spans[0])
    use_sibling(0)
    for q in range(1, n_piece):
        arrive(q)
        if q > 1:
            use_sibling(q - 1)
        use_pair(last, core, *spans[q])
    use_sibling(n_piece - 1)
    for q in range(n_piece):
        sent(ring_send, last, q, False)
        sent(sib_send, last, q, False)


def solution(mesh):
    n_dev = mesh.shape["sp"]
    n_step = n_dev // 2 - 1
    row_spec = P(("dp", "sp"), None)

    def local_fn(z_rows, x_rows, v_rows, mask_row, length_scale, out_scale):
        mz, d = z_rows.shape
        nx, r = v_rows.shape
        slot_rows = nx // 2 + r * nx // 2 // d
        dma = pltpu.SemaphoreType.DMA
        y_t = pl.pallas_call(
            functools.partial(kernel, n_dev),
            name="ring_predict",
            out_shape=pltpu.VMEM((r, mz), F32),
            in_specs=[pl.BlockSpec(memory_space=pl.ANY)] * 4 + [pl.BlockSpec(memory_space=pltpu.SMEM)] * 2,
            out_specs=pl.BlockSpec(memory_space=pltpu.VMEM),
            scratch_shapes=[
                pltpu.VMEM((mz, d), BF16),
                pltpu.VMEM((d, mz), BF16),
                pltpu.VMEM((n_dev, 2, slot_rows, d), BF16),
                pltpu.VMEM((8, mz), F32),
                pltpu.VMEM((8, TILE), F32),
                pltpu.SMEM((1, n_dev), jnp.int32),
                pltpu.VMEM((nx, LANES), F32),
                dma((8,)),
                dma((2, n_step, 3)), dma((2, n_step, 3)),
                dma((2, n_step, 3)), dma((2, n_step, 3)),
                dma((2,)), dma((2,)),
            ],
            compiler_params=pltpu.CompilerParams(
                collective_id=0, has_side_effects=True,  vmem_limit_bytes=60 * 1024 * 1024),
        )(z_rows, x_rows, v_rows.T, mask_row, length_scale, out_scale)
        return y_t.T

    return jax.shard_map(local_fn, mesh=mesh, in_specs=(row_spec, row_spec, row_spec, row_spec, P(None), P(None)), out_specs=row_spec, check_vma=False)
```

```python
import functools
import math

import jax
import jax.numpy as jnp
from jax import lax
from jax.experimental import pallas as pl
from jax.experimental.pallas import tpu as pltpu
from jax.sharding import PartitionSpec as P

F32 = jnp.float32
BF16 = jnp.bfloat16
MESH = pl.DeviceIdType.MESH
LOG2_E = math.log2(math.e)
TILE = 512
LANES = 128


def kernel(n_dev, z_hbm, x_hbm, v_hbm, mask_hbm, ell_s, scl_s, y_ref,
           z_in, zt, xs, nzh, crow, mask_s, nx_s,
           load_sem, ring_send, ring_recv, sib_send, sib_recv, own_send, own_recv):
    n_chip = n_dev // 2
    n_step = n_chip - 1
    mz, d = z_hbm.shape
    r, nx = v_hbm.shape
    half_rows = nx // 2
    vrows = r * half_rows // d
    spans = ((0, half_rows // 2), (half_rows // 2, 5 * half_rows // 16), (13 * half_rows // 16, 3 * half_rows // 16))
    n_piece = len(spans)
    last = n_step - 1

    me = lax.axis_index("sp")
    chip, core = me // 2, me % 2
    right = ((chip + 1) % n_chip) * 2 + core
    left = ((chip + n_chip - 1) % n_chip) * 2 + core
    sib = chip * 2 + (1 - core)

    barrier = pltpu.get_barrier_semaphore()
    for peer in (right, left, sib):
        pl.semaphore_signal(barrier, inc=1, device_id={"sp": peer}, device_id_type=MESH)

    loads = [pltpu.make_async_copy(x_hbm.at[pl.ds(half * half_rows, half_rows)],
                                   xs.at[me, half, pl.ds(vrows, half_rows)], load_sem.at[half]) for half in range(2)]
    loads += [pltpu.make_async_copy(v_hbm.at[pl.ds(b * vrows, vrows), pl.ds(half * half_rows, half_rows)],
                                    xs.at[me, half, pl.ds(0, vrows), pl.ds(b * half_rows, half_rows)],
                                    load_sem.at[2 + 2 * half + b]) for half in range(2) for b in range(2)]
    n_own = len(loads)
    loads += [
        pltpu.make_async_copy(mask_hbm, mask_s, load_sem.at[n_own]),
        pltpu.make_async_copy(z_hbm, z_in, load_sem.at[n_own + 1]),
    ]
    for load in loads:
        load.start()

    def remote(src_dst, send_sem, recv_sem, peer):
        return pltpu.make_async_remote_copy(
            src_ref=src_dst, dst_ref=src_dst, send_sem=send_sem, recv_sem=recv_sem,
            device_id={"sp": peer}, device_id_type=MESH)

    def piece(j, half, q, whole):
        if whole:
            return xs.at[j, half]
        lo, rows = spans[q]
        return xs.at[j, half, pl.ds(vrows + lo, rows) if q else pl.ds(0, vrows + rows)]

    def to_right(s, q=0, whole=True):
        j = ((chip + n_chip - s // 2) % n_chip) * 2 + core
        return remote(piece(j, s % 2, q, whole), ring_send.at[0, s, q], ring_recv.at[0, s, q], right)

    def to_left(s, q=0, whole=True):
        j = ((chip + s // 2) % n_chip) * 2 + core
        return remote(piece(j, 1 - s % 2, q, whole), ring_send.at[1, s, q], ring_recv.at[1, s, q], left)

    def source(u, c):
        h = u // 2 + 1
        return (((chip + n_chip - h) % n_chip) * 2 + c, u % 2), (((chip + h) % n_chip) * 2 + c, 1 - u % 2)

    def from_ring(u, q=0, whole=True):
        a, b = source(u, core)
        return (remote(piece(*a, q, whole), ring_send.at[0, u, q], ring_recv.at[0, u, q], left),
                remote(piece(*b, q, whole), ring_send.at[1, u, q], ring_recv.at[1, u, q], right))

    def sibling(u, c, q=0, whole=True):
        a, b = source(u, c)
        return (remote(piece(*a, q, whole), sib_send.at[0, u, q], sib_recv.at[0, u, q], sib),
                remote(piece(*b, q, whole), sib_send.at[1, u, q], sib_recv.at[1, u, q], sib))

    def own(j, half):
        return remote(xs.at[j, half], own_send.at[half], own_recv.at[half], sib)

    def sent(sems, u, q=0, whole=True):
        for k in range(2):
            remote(piece(0, 0, q, whole), sems.at[k, u, q], ring_recv.at[k, u, q], sib).wait_send()

    for load in loads[:n_own]:
        load.wait()
    pl.semaphore_wait(barrier, 3)
    for s in range(2):
        to_right(s).start()
        to_left(s).start()
    for half in range(2):
        own(me, half).start()

    for load in loads[n_own:]:
        load.wait()
    ell = jnp.full((8, TILE), ell_s[0], F32)
    crow[...] = (-LOG2_E) / (ell * ell)
    for t in range(mz // TILE):
        zt_t = z_in[t * TILE:(t + 1) * TILE, :].T
        zt[:, t * TILE:(t + 1) * TILE] = zt_t
        zf = zt_t.astype(F32)
        nzh[:, t * TILE:(t + 1) * TILE] = jnp.broadcast_to(
            0.5 * jnp.sum(zf * zf, axis=0, keepdims=True), (8, TILE))
    y_ref[...] = jnp.zeros_like(y_ref)

    def weighted(j, half, lo, rows):
        v_rows = jnp.concatenate(
            [xs[j, half, 0:vrows, b * half_rows:(b + 1) * half_rows][:, lo:lo + rows] for b in range(r // vrows)], axis=0)
        return (v_rows.astype(F32) * mask_s[0, j].astype(F32)).astype(BF16)

    def accumulate(x, vt_x):
        rows = x.shape[0]
        xf = x.astype(F32)
        nx_s[0:rows, :] = jnp.broadcast_to(0.5 * jnp.sum(xf * xf, axis=1, keepdims=True), (rows, LANES))
        scale = scl_s[0]
        tiles = [slice(t * TILE, (t + 1) * TILE) for t in range(mz // TILE)]
        ahead = jnp.dot(x, zt[:, tiles[0]], preferred_element_type=F32)
        for t, cols in enumerate(tiles):
            gram = ahead
            if t + 1 < len(tiles):
                ahead = jnp.dot(x, zt[:, tiles[t + 1]], preferred_element_type=F32)
            nxh = jnp.concatenate([nx_s[0:rows, :]] * (TILE // LANES), axis=1)
            half_dist = jnp.maximum(nzh[0:1, cols] + nxh - gram, 0.0)
            kern = (scale * jnp.exp2(half_dist * crow[0:1, :])).astype(BF16)
            y_ref[:, cols] += jnp.dot(vt_x, kern, preferred_element_type=F32)

    def use_halves(*blocks):
        x = jnp.concatenate([xs[j, half, vrows:vrows + half_rows, :] for j, half in blocks], axis=0)
        accumulate(x, jnp.concatenate([weighted(j, half, 0, half_rows) for j, half in blocks], axis=1))

    def use_pair(u, c, lo, rows):
        a, b = source(u, c)
        x = jnp.concatenate([xs[a[0], a[1], pl.ds(vrows + lo, rows), :], xs[b[0], b[1], pl.ds(vrows + lo, rows), :]], axis=0)
        accumulate(x, jnp.concatenate([weighted(*a, lo, rows), weighted(*b, lo, rows)], axis=1))

    use_halves((me, 0), (me, 1))
    for half in range(2):
        own(sib, half).wait_recv()
    use_halves((sib, 0), (sib, 1))

    @pl.loop(0, last)
    def _(u):
        ring, to_sib = from_ring(u), sibling(u, core)
        for k in range(2):
            onward = (to_right, to_left)[k]
            ring[k].wait_recv()

            @pl.when(u < last - 2)
            def _():
                onward(u + 2).start()

            @pl.when(u == last - 2)
            def _():
                for q in range(n_piece):
                    onward(last, q, False).start()

            to_sib[k].start()
        use_halves(*source(u, core))
        for copy in sibling(u, 1 - core):
            copy.wait_recv()
        use_halves(*source(u, 1 - core))

    def arrive(q):
        ring, to_sib = from_ring(last, q, False), sibling(last, core, q, False)
        for k in range(2):
            ring[k].wait_recv()
            to_sib[k].start()

    def use_sibling(q):
        for copy in sibling(last, 1 - core, q, False):
            copy.wait_recv()
        use_pair(last, 1 - core, *spans[q])

    arrive(0)
    use_pair(last, core, *spans[0])
    use_sibling(0)
    for q in range(1, n_piece):
        arrive(q)
        if q > 1:
            use_sibling(q - 1)
        use_pair(last, core, *spans[q])
    use_sibling(n_piece - 1)
    for half in range(2):
        own(me, half).wait_send()
    for u in range(last):
        sent(ring_send, u)
        sent(sib_send, u)
    for q in range(n_piece):
        sent(ring_send, last, q, False)
        sent(sib_send, last, q, False)


def solution(mesh):
    n_dev = mesh.shape["sp"]
    n_step = n_dev // 2 - 1
    row_spec = P(("dp", "sp"), None)

    def local_fn(z_rows, x_rows, v_rows, mask_row, length_scale, out_scale):
        mz, d = z_rows.shape
        nx, r = v_rows.shape
        slot_rows = nx // 2 + r * nx // 2 // d
        dma = pltpu.SemaphoreType.DMA
        y_t = pl.pallas_call(
            functools.partial(kernel, n_dev),
            name="ring_predict",
            out_shape=pltpu.VMEM((r, mz), F32),
            in_specs=[pl.BlockSpec(memory_space=pl.ANY)] * 4 + [pl.BlockSpec(memory_space=pltpu.SMEM)] * 2,
            out_specs=pl.BlockSpec(memory_space=pltpu.VMEM),
            scratch_shapes=[
                pltpu.VMEM((mz, d), BF16),
                pltpu.VMEM((d, mz), BF16),
                pltpu.VMEM((n_dev, 2, slot_rows, d), BF16),
                pltpu.VMEM((8, mz), F32),
                pltpu.VMEM((8, TILE), F32),
                pltpu.SMEM((1, n_dev), jnp.int32),
                pltpu.VMEM((nx, LANES), F32),
                dma((8,)),
                dma((2, n_step, 3)), dma((2, n_step, 3)),
                dma((2, n_step, 3)), dma((2, n_step, 3)),
                dma((2,)), dma((2,)),
            ],
            compiler_params=pltpu.CompilerParams(
                collective_id=0, has_side_effects=True,  vmem_limit_bytes=60 * 1024 * 1024),
        )(z_rows, x_rows, v_rows.T, mask_row, length_scale, out_scale)
        return y_t.T

    return jax.shard_map(local_fn, mesh=mesh, in_specs=(row_spec, row_spec, row_spec, row_spec, P(None), P(None)), out_specs=row_spec, check_vma=False)
```

```python
import functools
import math

import jax
import jax.numpy as jnp
from jax import lax
from jax.experimental import pallas as pl
from jax.experimental.pallas import tpu as pltpu
from jax.sharding import PartitionSpec as P

F32 = jnp.float32
BF16 = jnp.bfloat16
MESH = pl.DeviceIdType.MESH
LOG2_E = math.log2(math.e)
TILE = 512
LANES = 128


def kernel(n_dev, z_hbm, x_hbm, v_hbm, mask_hbm, ell_s, scl_s, y_ref,
           z_in, zt, xs, nzh, crow, mask_s, nx_s,
           load_sem, ring_send, ring_recv, sib_send, sib_recv, own_send, own_recv):
    n_chip = n_dev // 2
    n_step = n_chip - 1
    mz, d = z_hbm.shape
    r, nx = v_hbm.shape
    half_rows = nx // 2
    vrows = r * half_rows // d
    spans = ((0, half_rows // 2), (half_rows // 2, half_rows // 2))
    n_piece = len(spans)

    me = lax.axis_index("sp")
    chip, core = me // 2, me % 2
    right = ((chip + 1) % n_chip) * 2 + core
    left = ((chip + n_chip - 1) % n_chip) * 2 + core
    sib = chip * 2 + (1 - core)

    barrier = pltpu.get_barrier_semaphore()
    for peer in (right, left, sib):
        pl.semaphore_signal(barrier, inc=1, device_id={"sp": peer}, device_id_type=MESH)

    loads = [pltpu.make_async_copy(x_hbm.at[pl.ds(half * half_rows, half_rows)],
                                   xs.at[me, half, pl.ds(vrows, half_rows)], load_sem.at[half]) for half in range(2)]
    loads += [pltpu.make_async_copy(v_hbm.at[pl.ds(b * vrows, vrows), pl.ds(half * half_rows, half_rows)],
                                    xs.at[me, half, pl.ds(0, vrows), pl.ds(b * half_rows, half_rows)],
                                    load_sem.at[2 + 2 * half + b]) for half in range(2) for b in range(2)]
    n_own = len(loads)
    loads += [
        pltpu.make_async_copy(mask_hbm, mask_s, load_sem.at[n_own]),
        pltpu.make_async_copy(z_hbm, z_in, load_sem.at[n_own + 1]),
    ]
    for load in loads:
        load.start()

    def remote(src_dst, send_sem, recv_sem, peer):
        return pltpu.make_async_remote_copy(
            src_ref=src_dst, dst_ref=src_dst, send_sem=send_sem, recv_sem=recv_sem,
            device_id={"sp": peer}, device_id_type=MESH)

    def piece(j, half, q):
        lo, rows = spans[q]
        return xs.at[j, half, pl.ds(vrows + lo, rows) if q else pl.ds(0, vrows + rows)]

    def to_right(s, q):
        j = ((chip + n_chip - s // 2) % n_chip) * 2 + core
        return remote(piece(j, s % 2, q), ring_send.at[0, s, q], ring_recv.at[0, s, q], right)

    def to_left(s, q):
        j = ((chip + s // 2) % n_chip) * 2 + core
        return remote(piece(j, 1 - s % 2, q), ring_send.at[1, s, q], ring_recv.at[1, s, q], left)

    def source(u, c):
        h = u // 2 + 1
        return (((chip + n_chip - h) % n_chip) * 2 + c, u % 2), (((chip + h) % n_chip) * 2 + c, 1 - u % 2)

    def from_ring(u, q):
        a, b = source(u, core)
        return (remote(piece(*a, q), ring_send.at[0, u, q], ring_recv.at[0, u, q], left),
                remote(piece(*b, q), ring_send.at[1, u, q], ring_recv.at[1, u, q], right))

    def sibling(u, c, q):
        a, b = source(u, c)
        return (remote(piece(*a, q), sib_send.at[0, u, q], sib_recv.at[0, u, q], sib),
                remote(piece(*b, q), sib_send.at[1, u, q], sib_recv.at[1, u, q], sib))

    def own(j, half):
        return remote(xs.at[j, half], own_send.at[half], own_recv.at[half], sib)

    def sent(sems, u, q):
        for k in range(2):
            remote(piece(0, 0, q), sems.at[k, u, q], ring_recv.at[k, u, q], sib).wait_send()

    for load in loads[:n_own]:
        load.wait()
    pl.semaphore_wait(barrier, 3)
    for s in range(2):
        for q in range(n_piece):
            to_right(s, q).start()
            to_left(s, q).start()
    for half in range(2):
        own(me, half).start()

    for load in loads[n_own:]:
        load.wait()
    ell = jnp.full((8, TILE), ell_s[0], F32)
    crow[...] = (-LOG2_E) / (ell * ell)
    for t in range(mz // TILE):
        zt_t = z_in[t * TILE:(t + 1) * TILE, :].T
        zt[:, t * TILE:(t + 1) * TILE] = zt_t
        zf = zt_t.astype(F32)
        nzh[:, t * TILE:(t + 1) * TILE] = jnp.broadcast_to(
            0.5 * jnp.sum(zf * zf, axis=0, keepdims=True), (8, TILE))
    y_ref[...] = jnp.zeros_like(y_ref)

    def weighted(j, half, lo, rows):
        v_rows = jnp.concatenate(
            [xs[j, half, 0:vrows, b * half_rows:(b + 1) * half_rows][:, lo:lo + rows] for b in range(r // vrows)], axis=0)
        return (v_rows.astype(F32) * mask_s[0, j].astype(F32)).astype(BF16)

    def accumulate(x, vt_x):
        rows = x.shape[0]
        xf = x.astype(F32)
        nx_s[0:rows, :] = jnp.broadcast_to(0.5 * jnp.sum(xf * xf, axis=1, keepdims=True), (rows, LANES))
        scale = scl_s[0]
        tiles = [slice(t * TILE, (t + 1) * TILE) for t in range(mz // TILE)]
        ahead = jnp.dot(x, zt[:, tiles[0]], preferred_element_type=F32)
        for t, cols in enumerate(tiles):
            gram = ahead
            if t + 1 < len(tiles):
                ahead = jnp.dot(x, zt[:, tiles[t + 1]], preferred_element_type=F32)
            nxh = jnp.concatenate([nx_s[0:rows, :]] * (TILE // LANES), axis=1)
            half_dist = jnp.maximum(nzh[0:1, cols] + nxh - gram, 0.0)
            kern = (scale * jnp.exp2(half_dist * crow[0:1, :])).astype(BF16)
            y_ref[:, cols] += jnp.dot(vt_x, kern, preferred_element_type=F32)

    def use_halves(*blocks):
        x = jnp.concatenate([xs[j, half, vrows:vrows + half_rows, :] for j, half in blocks], axis=0)
        accumulate(x, jnp.concatenate([weighted(j, half, 0, half_rows) for j, half in blocks], axis=1))

    def use_pair(u, c, lo, rows):
        a, b = source(u, c)
        x = jnp.concatenate([xs[a[0], a[1], pl.ds(vrows + lo, rows), :], xs[b[0], b[1], pl.ds(vrows + lo, rows), :]], axis=0)
        accumulate(x, jnp.concatenate([weighted(*a, lo, rows), weighted(*b, lo, rows)], axis=1))

    use_halves((me, 0), (me, 1))
    for half in range(2):
        own(sib, half).wait_recv()
    use_halves((sib, 0), (sib, 1))

    @pl.loop(0, n_step)
    def _(u):
        for q in range(n_piece):
            ring, to_sib = from_ring(u, q), sibling(u, core, q)
            for k in range(2):
                ring[k].wait_recv()

                @pl.when(u < n_step - 2)
                def _():
                    (to_right, to_left)[k](u + 2, q).start()

                to_sib[k].start()
            use_pair(u, core, *spans[q])
            for copy in sibling(u, 1 - core, q):
                copy.wait_recv()
            use_pair(u, 1 - core, *spans[q])

    for half in range(2):
        own(me, half).wait_send()
    for u in range(n_step):
        for q in range(n_piece):
            sent(ring_send, u, q)
            sent(sib_send, u, q)


def solution(mesh):
    n_dev = mesh.shape["sp"]
    n_step = n_dev // 2 - 1
    row_spec = P(("dp", "sp"), None)

    def local_fn(z_rows, x_rows, v_rows, mask_row, length_scale, out_scale):
        mz, d = z_rows.shape
        nx, r = v_rows.shape
        slot_rows = nx // 2 + r * nx // 2 // d
        dma = pltpu.SemaphoreType.DMA
        y_t = pl.pallas_call(
            functools.partial(kernel, n_dev),
            name="ring_predict",
            out_shape=pltpu.VMEM((r, mz), F32),
            in_specs=[pl.BlockSpec(memory_space=pl.ANY)] * 4 + [pl.BlockSpec(memory_space=pltpu.SMEM)] * 2,
            out_specs=pl.BlockSpec(memory_space=pltpu.VMEM),
            scratch_shapes=[
                pltpu.VMEM((mz, d), BF16),
                pltpu.VMEM((d, mz), BF16),
                pltpu.VMEM((n_dev, 2, slot_rows, d), BF16),
                pltpu.VMEM((8, mz), F32),
                pltpu.VMEM((8, TILE), F32),
                pltpu.SMEM((1, n_dev), jnp.int32),
                pltpu.VMEM((nx, LANES), F32),
                dma((8,)),
                dma((2, n_step, 2)), dma((2, n_step, 2)),
                dma((2, n_step, 2)), dma((2, n_step, 2)),
                dma((2,)), dma((2,)),
            ],
            compiler_params=pltpu.CompilerParams(
                collective_id=0, has_side_effects=True,  vmem_limit_bytes=60 * 1024 * 1024),
        )(z_rows, x_rows, v_rows.T, mask_row, length_scale, out_scale)
        return y_t.T

    return jax.shard_map(local_fn, mesh=mesh, in_specs=(row_spec, row_spec, row_spec, row_spec, P(None), P(None)), out_specs=row_spec, check_vma=False)
```

```python
import functools
import math

import jax
import jax.numpy as jnp
from jax import lax
from jax.experimental import pallas as pl
from jax.experimental.pallas import tpu as pltpu
from jax.sharding import PartitionSpec as P

F32 = jnp.float32
BF16 = jnp.bfloat16
MESH = pl.DeviceIdType.MESH
LOG2_E = math.log2(math.e)
TILE = 512
LANES = 128


def kernel(n_dev, z_hbm, x_hbm, v_hbm, mask_hbm, ell_s, scl_s, y_ref,
           z_in, zt, xs, nzh, crow, mask_s, nx_s,
           load_sem, ring_send, ring_recv, sib_send, sib_recv, own_send, own_recv):
    n_chip = n_dev // 2
    n_step = n_chip - 1
    mz, d = z_hbm.shape
    r, nx = v_hbm.shape
    half_rows = nx // 2
    vrows = r * half_rows // d
    spans = ((0, half_rows // 2), (half_rows // 2, half_rows // 2))
    n_piece = len(spans)
    last = n_step - 1

    me = lax.axis_index("sp")
    chip, core = me // 2, me % 2
    right = ((chip + 1) % n_chip) * 2 + core
    left = ((chip + n_chip - 1) % n_chip) * 2 + core
    sib = chip * 2 + (1 - core)

    barrier = pltpu.get_barrier_semaphore()
    for peer in (right, left, sib):
        pl.semaphore_signal(barrier, inc=1, device_id={"sp": peer}, device_id_type=MESH)

    loads = [pltpu.make_async_copy(x_hbm.at[pl.ds(half * half_rows, half_rows)],
                                   xs.at[me, half, pl.ds(vrows, half_rows)], load_sem.at[half]) for half in range(2)]
    loads += [pltpu.make_async_copy(v_hbm.at[pl.ds(b * vrows, vrows), pl.ds(half * half_rows, half_rows)],
                                    xs.at[me, half, pl.ds(0, vrows), pl.ds(b * half_rows, half_rows)],
                                    load_sem.at[2 + 2 * half + b]) for half in range(2) for b in range(2)]
    n_own = len(loads)
    loads += [
        pltpu.make_async_copy(mask_hbm, mask_s, load_sem.at[n_own]),
        pltpu.make_async_copy(z_hbm, z_in, load_sem.at[n_own + 1]),
    ]
    for load in loads:
        load.start()

    def remote(src_dst, send_sem, recv_sem, peer):
        return pltpu.make_async_remote_copy(
            src_ref=src_dst, dst_ref=src_dst, send_sem=send_sem, recv_sem=recv_sem,
            device_id={"sp": peer}, device_id_type=MESH)

    def piece(j, half, q, whole):
        if whole:
            return xs.at[j, half]
        lo, rows = spans[q]
        return xs.at[j, half, pl.ds(vrows + lo, rows) if q else pl.ds(0, vrows + rows)]

    def to_right(s, q=0, whole=True):
        j = ((chip + n_chip - s // 2) % n_chip) * 2 + core
        return remote(piece(j, s % 2, q, whole), ring_send.at[0, s, q], ring_recv.at[0, s, q], right)

    def to_left(s, q=0, whole=True):
        j = ((chip + s // 2) % n_chip) * 2 + core
        return remote(piece(j, 1 - s % 2, q, whole), ring_send.at[1, s, q], ring_recv.at[1, s, q], left)

    def source(u, c):
        h = u // 2 + 1
        return (((chip + n_chip - h) % n_chip) * 2 + c, u % 2), (((chip + h) % n_chip) * 2 + c, 1 - u % 2)

    def from_ring(u, q=0, whole=True):
        a, b = source(u, core)
        return (remote(piece(*a, q, whole), ring_send.at[0, u, q], ring_recv.at[0, u, q], left),
                remote(piece(*b, q, whole), ring_send.at[1, u, q], ring_recv.at[1, u, q], right))

    def sibling(u, c, q=0, whole=True):
        a, b = source(u, c)
        return (remote(piece(*a, q, whole), sib_send.at[0, u, q], sib_recv.at[0, u, q], sib),
                remote(piece(*b, q, whole), sib_send.at[1, u, q], sib_recv.at[1, u, q], sib))

    def own(j, half):
        return remote(xs.at[j, half], own_send.at[half], own_recv.at[half], sib)

    def sent(sems, u, q=0, whole=True):
        for k in range(2):
            remote(piece(0, 0, q, whole), sems.at[k, u, q], ring_recv.at[k, u, q], sib).wait_send()

    for load in loads[:n_own]:
        load.wait()
    pl.semaphore_wait(barrier, 3)
    for s in range(2):
        to_right(s).start()
        to_left(s).start()
    for half in range(2):
        own(me, half).start()

    for load in loads[n_own:]:
        load.wait()
    ell = jnp.full((8, TILE), ell_s[0], F32)
    crow[...] = (-LOG2_E) / (ell * ell)
    for t in range(mz // TILE):
        zt_t = z_in[t * TILE:(t + 1) * TILE, :].T
        zt[:, t * TILE:(t + 1) * TILE] = zt_t
        zf = zt_t.astype(F32)
        nzh[:, t * TILE:(t + 1) * TILE] = jnp.broadcast_to(
            0.5 * jnp.sum(zf * zf, axis=0, keepdims=True), (8, TILE))
    y_ref[...] = jnp.zeros_like(y_ref)

    def weighted(j, half, lo, rows):
        v_rows = jnp.concatenate(
            [xs[j, half, 0:vrows, b * half_rows:(b + 1) * half_rows][:, lo:lo + rows] for b in range(r // vrows)], axis=0)
        return (v_rows.astype(F32) * mask_s[0, j].astype(F32)).astype(BF16)

    def accumulate(x, vt_x):
        rows = x.shape[0]
        xf = x.astype(F32)
        nx_s[0:rows, :] = jnp.broadcast_to(0.5 * jnp.sum(xf * xf, axis=1, keepdims=True), (rows, LANES))
        scale = scl_s[0]
        tiles = [slice(t * TILE, (t + 1) * TILE) for t in range(mz // TILE)]
        ahead = jnp.dot(x, zt[:, tiles[0]], preferred_element_type=F32)
        for t, cols in enumerate(tiles):
            gram = ahead
            if t + 1 < len(tiles):
                ahead = jnp.dot(x, zt[:, tiles[t + 1]], preferred_element_type=F32)
            nxh = jnp.concatenate([nx_s[0:rows, :]] * (TILE // LANES), axis=1)
            half_dist = jnp.maximum(nzh[0:1, cols] + nxh - gram, 0.0)
            kern = (scale * jnp.exp2(half_dist * crow[0:1, :])).astype(BF16)
            y_ref[:, cols] += jnp.dot(vt_x, kern, preferred_element_type=F32)

    def use_halves(*blocks):
        x = jnp.concatenate([xs[j, half, vrows:vrows + half_rows, :] for j, half in blocks], axis=0)
        accumulate(x, jnp.concatenate([weighted(j, half, 0, half_rows) for j, half in blocks], axis=1))

    def use_pair(u, c, lo, rows):
        a, b = source(u, c)
        x = jnp.concatenate([xs[a[0], a[1], pl.ds(vrows + lo, rows), :], xs[b[0], b[1], pl.ds(vrows + lo, rows), :]], axis=0)
        accumulate(x, jnp.concatenate([weighted(*a, lo, rows), weighted(*b, lo, rows)], axis=1))

    use_halves((me, 0), (me, 1))
    for half in range(2):
        own(sib, half).wait_recv()
    use_halves((sib, 0), (sib, 1))

    @pl.loop(0, last)
    def _(u):
        ring, to_sib = from_ring(u), sibling(u, core)
        for k in range(2):
            onward = (to_right, to_left)[k]
            ring[k].wait_recv()

            @pl.when(u < last - 2)
            def _():
                onward(u + 2).start()

            @pl.when(u == last - 2)
            def _():
                for q in range(n_piece):
                    onward(last, q, False).start()

            to_sib[k].start()
        use_halves(*source(u, core))
        for copy in sibling(u, 1 - core):
            copy.wait_recv()
        use_halves(*source(u, 1 - core))

        @pl.when(u > 0)
        def _():
            sent(ring_send, u - 1)
            sent(sib_send, u - 1)

    sent(ring_send, last - 1)
    sent(sib_send, last - 1)
    for half in range(2):
        own(me, half).wait_send()

    def arrive(q):
        ring, to_sib = from_ring(last, q, False), sibling(last, core, q, False)
        for k in range(2):
            ring[k].wait_recv()
            to_sib[k].start()

    def use_sibling(q):
        for copy in sibling(last, 1 - core, q, False):
            copy.wait_recv()
        use_pair(last, 1 - core, *spans[q])

    for q in range(n_piece):
        arrive(q)
        use_pair(last, core, *spans[q])
        use_sibling(q)
    for q in range(n_piece):
        sent(ring_send, last, q, False)
        sent(sib_send, last, q, False)


def solution(mesh):
    n_dev = mesh.shape["sp"]
    n_step = n_dev // 2 - 1
    row_spec = P(("dp", "sp"), None)

    def local_fn(z_rows, x_rows, v_rows, mask_row, length_scale, out_scale):
        mz, d = z_rows.shape
        nx, r = v_rows.shape
        slot_rows = nx // 2 + r * nx // 2 // d
        dma = pltpu.SemaphoreType.DMA
        y_t = pl.pallas_call(
            functools.partial(kernel, n_dev),
            name="ring_predict",
            out_shape=pltpu.VMEM((r, mz), F32),
            in_specs=[pl.BlockSpec(memory_space=pl.ANY)] * 4 + [pl.BlockSpec(memory_space=pltpu.SMEM)] * 2,
            out_specs=pl.BlockSpec(memory_space=pltpu.VMEM),
            scratch_shapes=[
                pltpu.VMEM((mz, d), BF16),
                pltpu.VMEM((d, mz), BF16),
                pltpu.VMEM((n_dev, 2, slot_rows, d), BF16),
                pltpu.VMEM((8, mz), F32),
                pltpu.VMEM((8, TILE), F32),
                pltpu.SMEM((1, n_dev), jnp.int32),
                pltpu.VMEM((nx, LANES), F32),
                dma((8,)),
                dma((2, n_step, 2)), dma((2, n_step, 2)),
                dma((2, n_step, 2)), dma((2, n_step, 2)),
                dma((2,)), dma((2,)),
            ],
            compiler_params=pltpu.CompilerParams(
                collective_id=0, has_side_effects=True,  vmem_limit_bytes=60 * 1024 * 1024),
        )(z_rows, x_rows, v_rows.T, mask_row, length_scale, out_scale)
        return y_t.T

    return jax.shard_map(local_fn, mesh=mesh, in_specs=(row_spec, row_spec, row_spec, row_spec, P(None), P(None)), out_specs=row_spec, check_vma=False)
```

```python
import functools
import math

import jax
import jax.numpy as jnp
from jax import lax
from jax.experimental import pallas as pl
from jax.experimental.pallas import tpu as pltpu
from jax.sharding import PartitionSpec as P

F32 = jnp.float32
BF16 = jnp.bfloat16
MESH = pl.DeviceIdType.MESH
LOG2_E = math.log2(math.e)
TILE = 512
LANES = 128


def kernel(n_dev, z_hbm, x_hbm, v_hbm, mask_hbm, ell_s, scl_s, y_ref,
           z_in, zt, xs, nzh, crow, mask_s, nx_s,
           load_sem, ring_send, ring_recv, sib_send, sib_recv, own_send, own_recv):
    n_chip = n_dev // 2
    n_step = n_chip - 1
    mz, d = z_hbm.shape
    r, nx = v_hbm.shape
    half_rows = nx // 2
    vrows = r * half_rows // d
    n_piece = 4
    rows_piece = half_rows // n_piece
    spans = tuple((q * rows_piece, rows_piece) for q in range(n_piece))

    me = lax.axis_index("sp")
    chip, core = me // 2, me % 2
    right = ((chip + 1) % n_chip) * 2 + core
    left = ((chip + n_chip - 1) % n_chip) * 2 + core
    sib = chip * 2 + (1 - core)

    barrier = pltpu.get_barrier_semaphore()
    for peer in (right, left, sib):
        pl.semaphore_signal(barrier, inc=1, device_id={"sp": peer}, device_id_type=MESH)

    loads = [pltpu.make_async_copy(x_hbm.at[pl.ds(half * half_rows, half_rows)],
                                   xs.at[me, half, pl.ds(vrows, half_rows)], load_sem.at[half]) for half in range(2)]
    loads += [pltpu.make_async_copy(v_hbm.at[pl.ds(b * vrows, vrows), pl.ds(half * half_rows, half_rows)],
                                    xs.at[me, half, pl.ds(0, vrows), pl.ds(b * half_rows, half_rows)],
                                    load_sem.at[2 + 2 * half + b]) for half in range(2) for b in range(2)]
    n_own = len(loads)
    loads += [
        pltpu.make_async_copy(mask_hbm, mask_s, load_sem.at[n_own]),
        pltpu.make_async_copy(z_hbm, z_in, load_sem.at[n_own + 1]),
    ]
    for load in loads:
        load.start()

    def remote(src_dst, send_sem, recv_sem, peer):
        return pltpu.make_async_remote_copy(
            src_ref=src_dst, dst_ref=src_dst, send_sem=send_sem, recv_sem=recv_sem,
            device_id={"sp": peer}, device_id_type=MESH)

    def piece(j, half, q):
        lo, rows = spans[q]
        return xs.at[j, half, pl.ds(vrows + lo, rows) if q else pl.ds(0, vrows + rows)]

    def to_right(s, q):
        j = ((chip + n_chip - s // 2) % n_chip) * 2 + core
        return remote(piece(j, s % 2, q), ring_send.at[0, s, q], ring_recv.at[0, s, q], right)

    def to_left(s, q):
        j = ((chip + s // 2) % n_chip) * 2 + core
        return remote(piece(j, 1 - s % 2, q), ring_send.at[1, s, q], ring_recv.at[1, s, q], left)

    def source(u, c):
        h = u // 2 + 1
        return (((chip + n_chip - h) % n_chip) * 2 + c, u % 2), (((chip + h) % n_chip) * 2 + c, 1 - u % 2)

    def from_ring(u, q):
        a, b = source(u, core)
        return (remote(piece(*a, q), ring_send.at[0, u, q], ring_recv.at[0, u, q], left),
                remote(piece(*b, q), ring_send.at[1, u, q], ring_recv.at[1, u, q], right))

    def sibling(u, c, q):
        a, b = source(u, c)
        return (remote(piece(*a, q), sib_send.at[0, u, q], sib_recv.at[0, u, q], sib),
                remote(piece(*b, q), sib_send.at[1, u, q], sib_recv.at[1, u, q], sib))

    def own(j, half):
        return remote(xs.at[j, half], own_send.at[half], own_recv.at[half], sib)

    def sent(sems, u, q):
        for k in range(2):
            remote(piece(0, 0, q), sems.at[k, u, q], ring_recv.at[k, u, q], sib).wait_send()

    for load in loads[:n_own]:
        load.wait()
    pl.semaphore_wait(barrier, 3)
    for s in range(2):
        for q in range(n_piece):
            to_right(s, q).start()
            to_left(s, q).start()
    for half in range(2):
        own(me, half).start()

    for load in loads[n_own:]:
        load.wait()
    ell = jnp.full((8, TILE), ell_s[0], F32)
    crow[...] = (-LOG2_E) / (ell * ell)
    for t in range(mz // TILE):
        zt_t = z_in[t * TILE:(t + 1) * TILE, :].T
        zt[:, t * TILE:(t + 1) * TILE] = zt_t
        zf = zt_t.astype(F32)
        nzh[:, t * TILE:(t + 1) * TILE] = jnp.broadcast_to(
            0.5 * jnp.sum(zf * zf, axis=0, keepdims=True), (8, TILE))
    y_ref[...] = jnp.zeros_like(y_ref)

    def weighted(j, half, lo, rows):
        v_rows = jnp.concatenate(
            [xs[j, half, 0:vrows, b * half_rows:(b + 1) * half_rows][:, lo:lo + rows] for b in range(r // vrows)], axis=0)
        return (v_rows.astype(F32) * mask_s[0, j].astype(F32)).astype(BF16)

    def accumulate(x, vt_x):
        rows = x.shape[0]
        xf = x.astype(F32)
        nx_s[0:rows, :] = jnp.broadcast_to(0.5 * jnp.sum(xf * xf, axis=1, keepdims=True), (rows, LANES))
        scale = scl_s[0]
        tiles = [slice(t * TILE, (t + 1) * TILE) for t in range(mz // TILE)]
        ahead = jnp.dot(x, zt[:, tiles[0]], preferred_element_type=F32)
        for t, cols in enumerate(tiles):
            gram = ahead
            if t + 1 < len(tiles):
                ahead = jnp.dot(x, zt[:, tiles[t + 1]], preferred_element_type=F32)
            nxh = jnp.concatenate([nx_s[0:rows, :]] * (TILE // LANES), axis=1)
            half_dist = jnp.maximum(nzh[0:1, cols] + nxh - gram, 0.0)
            kern = (scale * jnp.exp2(half_dist * crow[0:1, :])).astype(BF16)
            y_ref[:, cols] += jnp.dot(vt_x, kern, preferred_element_type=F32)

    def use_halves(*blocks):
        x = jnp.concatenate([xs[j, half, vrows:vrows + half_rows, :] for j, half in blocks], axis=0)
        accumulate(x, jnp.concatenate([weighted(j, half, 0, half_rows) for j, half in blocks], axis=1))

    def use_pair(u, c, lo, rows):
        a, b = source(u, c)
        x = jnp.concatenate([xs[a[0], a[1], pl.ds(vrows + lo, rows), :], xs[b[0], b[1], pl.ds(vrows + lo, rows), :]], axis=0)
        accumulate(x, jnp.concatenate([weighted(*a, lo, rows), weighted(*b, lo, rows)], axis=1))

    use_halves((me, 0), (me, 1))
    for half in range(2):
        own(sib, half).wait_recv()
    use_halves((sib, 0), (sib, 1))

    @pl.loop(0, n_step)
    def _(u):
        for group in range(2):
            qs = (2 * group, 2 * group + 1)
            for q in qs:
                ring, to_sib = from_ring(u, q), sibling(u, core, q)
                for k in range(2):
                    ring[k].wait_recv()

                    @pl.when(u < n_step - 2)
                    def _():
                        (to_right, to_left)[k](u + 2, q).start()

                    to_sib[k].start()
            lo, rows = spans[qs[0]][0], 2 * rows_piece
            use_pair(u, core, lo, rows)
            for q in qs:
                for copy in sibling(u, 1 - core, q):
                    copy.wait_recv()
            use_pair(u, 1 - core, lo, rows)

    for half in range(2):
        own(me, half).wait_send()
    for u in range(n_step):
        for q in range(n_piece):
            sent(ring_send, u, q)
            sent(sib_send, u, q)


def solution(mesh):
    n_dev = mesh.shape["sp"]
    n_step = n_dev // 2 - 1
    row_spec = P(("dp", "sp"), None)

    def local_fn(z_rows, x_rows, v_rows, mask_row, length_scale, out_scale):
        mz, d = z_rows.shape
        nx, r = v_rows.shape
        slot_rows = nx // 2 + r * nx // 2 // d
        dma = pltpu.SemaphoreType.DMA
        y_t = pl.pallas_call(
            functools.partial(kernel, n_dev),
            name="ring_predict",
            out_shape=pltpu.VMEM((r, mz), F32),
            in_specs=[pl.BlockSpec(memory_space=pl.ANY)] * 4 + [pl.BlockSpec(memory_space=pltpu.SMEM)] * 2,
            out_specs=pl.BlockSpec(memory_space=pltpu.VMEM),
            scratch_shapes=[
                pltpu.VMEM((mz, d), BF16),
                pltpu.VMEM((d, mz), BF16),
                pltpu.VMEM((n_dev, 2, slot_rows, d), BF16),
                pltpu.VMEM((8, mz), F32),
                pltpu.VMEM((8, TILE), F32),
                pltpu.SMEM((1, n_dev), jnp.int32),
                pltpu.VMEM((nx, LANES), F32),
                dma((8,)),
                dma((2, n_step, 4)), dma((2, n_step, 4)),
                dma((2, n_step, 4)), dma((2, n_step, 4)),
                dma((2,)), dma((2,)),
            ],
            compiler_params=pltpu.CompilerParams(
                collective_id=0, has_side_effects=True, vmem_limit_bytes=60 * 1024 * 1024),
        )(z_rows, x_rows, v_rows.T, mask_row, length_scale, out_scale)
        return y_t.T

    return jax.shard_map(local_fn, mesh=mesh, in_specs=(row_spec, row_spec, row_spec, row_spec, P(None), P(None)), out_specs=row_spec, check_vma=False)
```

```python
import functools
import math

import jax
import jax.numpy as jnp
from jax import lax
from jax.experimental import pallas as pl
from jax.experimental.pallas import tpu as pltpu
from jax.sharding import PartitionSpec as P

F32 = jnp.float32
BF16 = jnp.bfloat16
MESH = pl.DeviceIdType.MESH
LOG2_E = math.log2(math.e)
TILE = 512
LANES = 128


def kernel(n_dev, z_hbm, x_hbm, v_hbm, mask_hbm, ell_s, scl_s, y_ref,
           z_in, zt, xs, nzh, crow, mask_s, nx_s,
           load_sem, ring_send, ring_recv, sib_send, sib_recv, own_send, own_recv):
    n_chip = n_dev // 2
    n_step = n_chip - 1
    mz, d = z_hbm.shape
    r, nx = v_hbm.shape
    half_rows = nx // 2
    vrows = r * half_rows // d
    spans = ((0, half_rows // 2), (half_rows // 2, half_rows // 2))
    n_piece = len(spans)
    last = n_step - 1

    me = lax.axis_index("sp")
    chip, core = me // 2, me % 2
    right = ((chip + 1) % n_chip) * 2 + core
    left = ((chip + n_chip - 1) % n_chip) * 2 + core
    sib = chip * 2 + (1 - core)

    barrier = pltpu.get_barrier_semaphore()
    for peer in (right, left, sib):
        pl.semaphore_signal(barrier, inc=1, device_id={"sp": peer}, device_id_type=MESH)

    loads = [pltpu.make_async_copy(x_hbm.at[pl.ds(half * half_rows, half_rows)],
                                   xs.at[me, half, pl.ds(vrows, half_rows)], load_sem.at[half]) for half in range(2)]
    loads += [pltpu.make_async_copy(v_hbm.at[pl.ds(b * vrows, vrows), pl.ds(half * half_rows, half_rows)],
                                    xs.at[me, half, pl.ds(0, vrows), pl.ds(b * half_rows, half_rows)],
                                    load_sem.at[2 + 2 * half + b]) for half in range(2) for b in range(2)]
    n_own = len(loads)
    loads += [
        pltpu.make_async_copy(mask_hbm, mask_s, load_sem.at[n_own]),
        pltpu.make_async_copy(z_hbm, z_in, load_sem.at[n_own + 1]),
    ]
    for load in loads:
        load.start()

    def remote(src_dst, send_sem, recv_sem, peer):
        return pltpu.make_async_remote_copy(
            src_ref=src_dst, dst_ref=src_dst, send_sem=send_sem, recv_sem=recv_sem,
            device_id={"sp": peer}, device_id_type=MESH)

    def piece(j, half, q, whole):
        if whole:
            return xs.at[j, half]
        lo, rows = spans[q]
        return xs.at[j, half, pl.ds(vrows + lo, rows) if q else pl.ds(0, vrows + rows)]

    def to_right(s, q=0, whole=True):
        j = ((chip + n_chip - s // 2) % n_chip) * 2 + core
        return remote(piece(j, s % 2, q, whole), ring_send.at[0, s, q], ring_recv.at[0, s, q], right)

    def to_left(s, q=0, whole=True):
        j = ((chip + s // 2) % n_chip) * 2 + core
        return remote(piece(j, 1 - s % 2, q, whole), ring_send.at[1, s, q], ring_recv.at[1, s, q], left)

    def source(u, c):
        h = u // 2 + 1
        return (((chip + n_chip - h) % n_chip) * 2 + c, u % 2), (((chip + h) % n_chip) * 2 + c, 1 - u % 2)

    def from_ring(u, q=0, whole=True):
        a, b = source(u, core)
        return (remote(piece(*a, q, whole), ring_send.at[0, u, q], ring_recv.at[0, u, q], left),
                remote(piece(*b, q, whole), ring_send.at[1, u, q], ring_recv.at[1, u, q], right))

    def sibling(u, c, q=0, whole=True):
        a, b = source(u, c)
        return (remote(piece(*a, q, whole), sib_send.at[0, u, q], sib_recv.at[0, u, q], sib),
                remote(piece(*b, q, whole), sib_send.at[1, u, q], sib_recv.at[1, u, q], sib))

    def own(j, half):
        return remote(xs.at[j, half], own_send.at[half], own_recv.at[half], sib)

    def sent(sems, u, q=0, whole=True):
        for k in range(2):
            remote(piece(0, 0, q, whole), sems.at[k, u, q], ring_recv.at[k, u, q], sib).wait_send()

    for load in loads[:n_own]:
        load.wait()
    pl.semaphore_wait(barrier, 3)
    for s in range(2):
        to_right(s).start()
        to_left(s).start()
    for half in range(2):
        own(me, half).start()

    for load in loads[n_own:]:
        load.wait()
    ell = jnp.full((8, TILE), ell_s[0], F32)
    crow[...] = (-LOG2_E) / (ell * ell)
    for t in range(mz // TILE):
        zt_t = z_in[t * TILE:(t + 1) * TILE, :].T
        zt[:, t * TILE:(t + 1) * TILE] = zt_t
        zf = zt_t.astype(F32)
        nzh[:, t * TILE:(t + 1) * TILE] = jnp.broadcast_to(
            0.5 * jnp.sum(zf * zf, axis=0, keepdims=True), (8, TILE))
    y_ref[...] = jnp.zeros_like(y_ref)

    def weighted(j, half, lo, rows):
        v_rows = jnp.concatenate(
            [xs[j, half, 0:vrows, b * half_rows:(b + 1) * half_rows][:, lo:lo + rows] for b in range(r // vrows)], axis=0)
        return (v_rows.astype(F32) * mask_s[0, j].astype(F32)).astype(BF16)

    def accumulate(x, vt_x):
        rows = x.shape[0]
        xf = x.astype(F32)
        nx_s[0:rows, :] = jnp.broadcast_to(0.5 * jnp.sum(xf * xf, axis=1, keepdims=True), (rows, LANES))
        scale = scl_s[0]
        tiles = [slice(t * TILE, (t + 1) * TILE) for t in range(mz // TILE)]
        ahead = jnp.dot(x, zt[:, tiles[0]], preferred_element_type=F32)
        for t, cols in enumerate(tiles):
            gram = ahead
            if t + 1 < len(tiles):
                ahead = jnp.dot(x, zt[:, tiles[t + 1]], preferred_element_type=F32)
            nxh = jnp.concatenate([nx_s[0:rows, :]] * (TILE // LANES), axis=1)
            half_dist = jnp.maximum(nzh[0:1, cols] + nxh - gram, 0.0)
            kern = (scale * jnp.exp2(half_dist * crow[0:1, :])).astype(BF16)
            y_ref[:, cols] += jnp.dot(vt_x, kern, preferred_element_type=F32)

    def use_halves(*blocks):
        x = jnp.concatenate([xs[j, half, vrows:vrows + half_rows, :] for j, half in blocks], axis=0)
        accumulate(x, jnp.concatenate([weighted(j, half, 0, half_rows) for j, half in blocks], axis=1))

    def use_pair(u, c, lo, rows):
        a, b = source(u, c)
        x = jnp.concatenate([xs[a[0], a[1], pl.ds(vrows + lo, rows), :], xs[b[0], b[1], pl.ds(vrows + lo, rows), :]], axis=0)
        accumulate(x, jnp.concatenate([weighted(*a, lo, rows), weighted(*b, lo, rows)], axis=1))

    use_halves((me, 0), (me, 1))
    for half in range(2):
        own(sib, half).wait_recv()
    use_halves((sib, 0), (sib, 1))

    @pl.loop(0, last)
    def _(u):
        ring, to_sib = from_ring(u), sibling(u, core)
        for k in range(2):
            onward = (to_right, to_left)[k]
            ring[k].wait_recv()

            @pl.when(u < last - 2)
            def _():
                onward(u + 2).start()

            @pl.when(u == last - 2)
            def _():
                for q in range(n_piece):
                    onward(last, q, False).start()

            to_sib[k].start()
        for span in spans:
            use_pair(u, core, *span)
        for copy in sibling(u, 1 - core):
            copy.wait_recv()
        for span in spans:
            use_pair(u, 1 - core, *span)

        @pl.when(u > 0)
        def _():
            sent(ring_send, u - 1)
            sent(sib_send, u - 1)

    sent(ring_send, last - 1)
    sent(sib_send, last - 1)
    for half in range(2):
        own(me, half).wait_send()

    def arrive(q):
        ring, to_sib = from_ring(last, q, False), sibling(last, core, q, False)
        for k in range(2):
            ring[k].wait_recv()
            to_sib[k].start()

    def use_sibling(q):
        for copy in sibling(last, 1 - core, q, False):
            copy.wait_recv()
        use_pair(last, 1 - core, *spans[q])

    for q in range(n_piece):
        arrive(q)
        use_pair(last, core, *spans[q])
        use_sibling(q)
    for q in range(n_piece):
        sent(ring_send, last, q, False)
        sent(sib_send, last, q, False)


def solution(mesh):
    n_dev = mesh.shape["sp"]
    n_step = n_dev // 2 - 1
    row_spec = P(("dp", "sp"), None)

    def local_fn(z_rows, x_rows, v_rows, mask_row, length_scale, out_scale):
        mz, d = z_rows.shape
        nx, r = v_rows.shape
        slot_rows = nx // 2 + r * nx // 2 // d
        dma = pltpu.SemaphoreType.DMA
        y_t = pl.pallas_call(
            functools.partial(kernel, n_dev),
            name="ring_predict",
            out_shape=pltpu.VMEM((r, mz), F32),
            in_specs=[pl.BlockSpec(memory_space=pl.ANY)] * 4 + [pl.BlockSpec(memory_space=pltpu.SMEM)] * 2,
            out_specs=pl.BlockSpec(memory_space=pltpu.VMEM),
            scratch_shapes=[
                pltpu.VMEM((mz, d), BF16),
                pltpu.VMEM((d, mz), BF16),
                pltpu.VMEM((n_dev, 2, slot_rows, d), BF16),
                pltpu.VMEM((8, mz), F32),
                pltpu.VMEM((8, TILE), F32),
                pltpu.SMEM((1, n_dev), jnp.int32),
                pltpu.VMEM((nx, LANES), F32),
                dma((8,)),
                dma((2, n_step, 2)), dma((2, n_step, 2)),
                dma((2, n_step, 2)), dma((2, n_step, 2)),
                dma((2,)), dma((2,)),
            ],
            compiler_params=pltpu.CompilerParams(
                collective_id=0, has_side_effects=True, vmem_limit_bytes=60 * 1024 * 1024),
        )(z_rows, x_rows, v_rows.T, mask_row, length_scale, out_scale)
        return y_t.T

    return jax.shard_map(local_fn, mesh=mesh, in_specs=(row_spec, row_spec, row_spec, row_spec, P(None), P(None)), out_specs=row_spec, check_vma=False)
```
